32 devices in a mesh: rep: 1 (over z), mp: 4 (over y), tb: 4 (over x), ta: 2 (over core).
Axes of the slice: x: 4, y: 4, z: 1, core: 2. Of those that a mesh axis runs over, the one named last changes fastest.
The devices are a block of a 4x4x8 slice.
Arguments:
- x_in: bfloat16 [512, 3072], P(('rep', 'tb', 'ta'), 'mp')
- seg_ids: int32 [512], P(('rep', 'tb', 'ta'))
- pos_ids: int32 [512], P(('rep', 'tb', 'ta'))
- w_q: bfloat16 [2, 3072, 4096], P(None, ('tb', 'ta'), 'mp')
- w_k: bfloat16 [2, 3072, 256], P(None, ('tb', 'ta'))
- w_v: bfloat16 [2, 3072, 256], P(None, ('tb', 'ta'))
- w_gate: bfloat16 [2, 3072, 24576], P(None, ('tb', 'ta'), 'mp')
- w_up: bfloat16 [2, 3072, 24576], P(None, ('tb', 'ta'), 'mp')
- w_out: bfloat16 [2, 4096, 3072], P(None, 'mp', ('tb', 'ta'))
- w_down: bfloat16 [2, 24576, 3072], P(None, 'mp', ('tb', 'ta'))
- norm_gain: bfloat16 [2, 3072], replicated
Outputs:
- output: float32 [512, 3072], P(('rep', 'tb', 'ta'), 'mp')
All inputs are finite; a program needn't handle non-finite values.
Results may differ from the reference program's by a relative error of at most 0.00926904.
Values are sent between devices in bfloat16 or wider.
A program may use at most 768 MiB of HBM per device.

```python
import jax
import jax.numpy as jnp
from jax import lax

TOKENS = 512
BLOCK_TOKENS = 64
EMBED = 3072
HEADS = 16
HEAD_DIM = 256
FFN_DIM = 24576
LAYERS = 2
NUM_BLOCKS = TOKENS // BLOCK_TOKENS
REQ_MEAN = max(2, min(BLOCK_TOKENS // 2, 64))
ROPE_BASE = 10000.0
NORM_EPS = 1e-6


def draw_requests(key):
    starts = jax.random.randint(key, (NUM_BLOCKS, BLOCK_TOKENS), 0, REQ_MEAN) == 0
    block_start = (jnp.arange(BLOCK_TOKENS) == 0)[None, :]
    start_flags = (starts | block_start).reshape(TOKENS).astype(jnp.int32)
    tok_index = jnp.arange(TOKENS, dtype=jnp.int32)
    seg_ids = jnp.cumsum(start_flags).astype(jnp.int32) - 1
    pos_ids = tok_index - lax.cummax(start_flags * tok_index, axis=0)
    return seg_ids, pos_ids


def normal_weight(key, shape, fan_in, scale_mult):
    return (jax.random.normal(key, shape, jnp.float32) * (scale_mult * fan_in ** -0.5)).astype(jnp.bfloat16)


def setup_inputs(seed: int = 0, part: int = 0) -> dict:
    part_key = jax.random.fold_in(jax.random.key(seed), part)
    key_x, key_req = jax.random.split(part_key)
    shared = jax.random.split(jax.random.key(seed + 1), 8)
    seg_ids, pos_ids = draw_requests(key_req)
    width_q = HEADS * HEAD_DIM
    return {
        "x_in": jax.random.normal(key_x, (TOKENS, EMBED), jnp.float32).astype(jnp.bfloat16),
        "seg_ids": seg_ids,
        "pos_ids": pos_ids,
        "w_q": normal_weight(shared[0], (LAYERS, EMBED, width_q), EMBED, 1.0),
        "w_k": normal_weight(shared[1], (LAYERS, EMBED, HEAD_DIM), EMBED, 1.0),
        "w_v": normal_weight(shared[2], (LAYERS, EMBED, HEAD_DIM), EMBED, 1.0),
        "w_gate": normal_weight(shared[3], (LAYERS, EMBED, FFN_DIM), EMBED, 1.0),
        "w_up": normal_weight(shared[4], (LAYERS, EMBED, FFN_DIM), EMBED, 1.0),
        "w_out": normal_weight(shared[5], (LAYERS, width_q, EMBED), width_q, 2.0),
        "w_down": normal_weight(shared[6], (LAYERS, FFN_DIM, EMBED), FFN_DIM, 1.0),
        "norm_gain": jax.random.uniform(shared[7], (LAYERS, EMBED), jnp.float32, 0.5, 1.5).astype(jnp.bfloat16),
    }


def apply_rope(rot_in, cos_tab, sin_tab):
    half_dim = HEAD_DIM // 2
    lower_half = rot_in[..., :half_dim].astype(jnp.float32)
    upper_half = rot_in[..., half_dim:].astype(jnp.float32)
    return jnp.concatenate([lower_half * cos_tab - upper_half * sin_tab, upper_half * cos_tab + lower_half * sin_tab], axis=-1).astype(jnp.bfloat16)


def layer_block(hidden, seg_blk, pos_blk, w_q, w_k, w_v, w_gate, w_up, w_out, w_down, gain):
    mean_sq = jnp.mean(hidden * hidden, axis=-1, keepdims=True)
    normed = (hidden * lax.rsqrt(mean_sq + NORM_EPS) * gain.astype(jnp.float32)).astype(jnp.bfloat16)
    q_proj = jnp.dot(normed, w_q, preferred_element_type=jnp.float32).astype(jnp.bfloat16)
    k_proj = jnp.dot(normed, w_k, preferred_element_type=jnp.float32).astype(jnp.bfloat16)
    v_proj = jnp.dot(normed, w_v, preferred_element_type=jnp.float32).astype(jnp.bfloat16)
    gate_proj = jnp.dot(normed, w_gate, preferred_element_type=jnp.float32).astype(jnp.bfloat16)
    up_proj = jnp.dot(normed, w_up, preferred_element_type=jnp.float32).astype(jnp.bfloat16)
    half_dim = HEAD_DIM // 2
    inv_freq = ROPE_BASE ** (-(jnp.arange(half_dim, dtype=jnp.float32) * 2.0) / HEAD_DIM)
    angles = pos_blk.astype(jnp.float32)[:, None] * inv_freq[None, :]
    cos_tab = jnp.cos(angles)
    sin_tab = jnp.sin(angles)
    q_rot = apply_rope(q_proj.reshape(BLOCK_TOKENS, HEADS, HEAD_DIM), cos_tab[:, None, :], sin_tab[:, None, :])
    k_rot = apply_rope(k_proj, cos_tab, sin_tab)
    allowed = (seg_blk[:, None] == seg_blk[None, :]) & (pos_blk[None, :] <= pos_blk[:, None])
    score_scale = HEAD_DIM ** -0.5

    def one_head(q_head):
        scores = jnp.dot(q_head, k_rot.T, preferred_element_type=jnp.float32) * score_scale
        scores = jnp.where(allowed, scores, -1e30)
        row_peak = jnp.max(scores, axis=-1, keepdims=True)
        exp_scores = jnp.exp(scores - row_peak)
        prob_bf16 = (exp_scores / jnp.sum(exp_scores, axis=-1, keepdims=True)).astype(jnp.bfloat16)
        return jnp.dot(prob_bf16, v_proj, preferred_element_type=jnp.float32).astype(jnp.bfloat16)

    attn_heads = lax.map(one_head, jnp.transpose(q_rot, (1, 0, 2)))
    attn = jnp.transpose(attn_heads, (1, 0, 2)).reshape(BLOCK_TOKENS, HEADS * HEAD_DIM)
    mlp_act = (jax.nn.silu(gate_proj.astype(jnp.float32)) * up_proj.astype(jnp.float32)).astype(jnp.bfloat16)
    branch = jnp.dot(attn, w_out, preferred_element_type=jnp.float32) + jnp.dot(mlp_act, w_down, preferred_element_type=jnp.float32)
    return hidden + branch


def reference(x_in, seg_ids, pos_ids, w_q, w_k, w_v, w_gate, w_up, w_out, w_down, norm_gain):
    seg_blocks = seg_ids.reshape(NUM_BLOCKS, BLOCK_TOKENS)
    pos_blocks = pos_ids.reshape(NUM_BLOCKS, BLOCK_TOKENS)

    def layer_step(hidden, weights):
        def block_step(blk):
            return layer_block(blk[0], blk[1], blk[2], weights[0], weights[1], weights[2], weights[3], weights[4], weights[5], weights[6], weights[7])

        hidden_blocks = lax.map(block_step, (hidden.reshape(NUM_BLOCKS, BLOCK_TOKENS, EMBED), seg_blocks, pos_blocks))
        return hidden_blocks.reshape(TOKENS, EMBED), None

    final_x, unused = lax.scan(layer_step, x_in.astype(jnp.float32), (w_q, w_k, w_v, w_gate, w_up, w_out, w_down, norm_gain))
    return final_x
```

```python
import functools

import jax
import jax.numpy as jnp
from jax import lax
from jax.experimental import pallas as pl
from jax.experimental.pallas import tpu as pltpu
from jax.sharding import PartitionSpec as P

ROPE_BASE = 10000.0
NORM_EPS = 1e-6
TOKEN_AXES = ("rep", "tb", "ta")
PLANE_AXES = ("tb", "ta")
MESH = pl.DeviceIdType.MESH
BF16, F32 = jnp.bfloat16, jnp.float32
NX, NY = 4, 4
CW = 256


def al(index, unit):
    return pl.multiple_of(index, unit)


def kernel(dims, x_ref, pack_ref, freq_ref, gain_ref, wq, wkv, wg, wu, wo, wd, out_ref,
           w_at, w_ml, wb, zs, zr, za, zar, m_buf, h_buf, acc, res, kv_buf, q_buf, cos_t, sin_t, packs,
           stat_own, stat_in, rs_in, x_in, f_in,
           xs_s, xs_r, ps_s, ps_r, w_s, wa_s, w_r, wa_r, wb_r, p_s, p_r, ring_s, ring_r, d_s, d_r,
           kv_s, kv_r, h_s, h_r, y_s, y_r, st_s, st_r, rs_s, rs_r, f_s, f_r):
    layers, blk, kw, gq, gkv, gff = dims
    nch = gff // CW
    tok = 8 * blk
    half = tok // 2
    tb2 = 2 * blk
    x, c, y = lax.axis_index("tb"), lax.axis_index("ta"), lax.axis_index("mp")
    right, left = (x + 1) % NX, (x + NX - 1) % NX
    nxt = right * (1 - c) + left * c
    group = (x + NX - c) % NX

    def dev(tb=None, ta=None, mp=None):
        return {"tb": x if tb is None else tb, "ta": c if ta is None else ta, "mp": y if mp is None else mp}

    sib = dev(ta=1 - c)
    ring = dev(tb=nxt)
    partner = dev(tb=nxt, ta=1 - c)

    def send(src, dst, ssem, rsem, to):
        pltpu.make_async_remote_copy(src_ref=src, dst_ref=dst, send_sem=ssem, recv_sem=rsem, device_id=to, device_id_type=MESH).start()

    def local(src, dst, sem):
        pltpu.make_async_copy(src, dst, sem).start()

    def wait(ref, sem):
        pltpu.make_async_copy(ref, ref, sem).wait()

    me_plane = 2 * x + c
    barrier = pltpu.get_barrier_semaphore()
    for d in range(1, 2 * NX):
        q = (me_plane + d) % (2 * NX)
        pl.semaphore_signal(barrier, inc=1, device_id=dev(tb=q // 2, ta=q % 2), device_id_type=MESH)
    for d in range(1, NY):
        pl.semaphore_signal(barrier, inc=1, device_id=dev(mp=(y + d) % NY), device_id_type=MESH)

    peers = 2 * NX - 1 + NY - 1

    @pl.when(x != y)
    def _():
        for t in range(2):
            pl.semaphore_signal(barrier, inc=1, device_id=dev(tb=y, ta=t, mp=x), device_id_type=MESH)
        pl.semaphore_wait(barrier, peers + 2)

    @pl.when(x == y)
    def _():
        pl.semaphore_wait(barrier, peers)

    def swap_start(src_of, dst, ssem, rsem):
        for t in range(2):
            own = jnp.logical_and(x == y, c == t)

            @pl.when(own)
            def _():
                local(src_of(t), dst, rsem.at[c])

            @pl.when(jnp.logical_not(own))
            def _():
                send(src_of(t), dst, ssem.at[t], rsem.at[c], dev(tb=y, ta=t, mp=x))

    def swap_wait(part, ssem, rsem):
        for t in range(2):
            wait(part, rsem.at[t])

            @pl.when(jnp.logical_not(jnp.logical_and(x == y, c == t)))
            def _():
                wait(part, ssem.at[t])

    swap_start(lambda t: x_ref.at[:, t * kw:(t + 1) * kw], x_in.at[pl.ds(al(c * blk, blk), blk)], xs_s, xs_r)

    pack_slot = (x % 2) * 2 + c
    pack_core = x // 2
    pack_own = c == pack_core

    @pl.when(pack_own)
    def _():
        local(pack_ref, packs.at[pack_slot], ps_r)

    @pl.when(jnp.logical_not(pack_own))
    def _():
        send(pack_ref, packs.at[pack_slot], ps_s.at[0], ps_r, dev(ta=pack_core))

    for d in range(1, NX):
        send(pack_ref, packs.at[pack_slot], ps_s.at[d], ps_r, dev(tb=(x + d) % NX, ta=pack_core))

    def issue_w(layer, idx):
        targets = (
            ((x + 1) % NX, c, dev(tb=right, ta=0)),
            ((x + 2) % NX, c, dev(tb=left, ta=1)),
            ((x + 3 + c) % NX, 2 + c, sib),
            (group, 2 + c, None),
        )
        for grp, slot, to in targets:
            rows = pl.ds(al(slot * kw, kw), kw)
            if idx == 0:
                pieces = (
                    (wq.at[layer, :, pl.ds(al(grp * gq, gq), gq)], w_at.at[layer, rows, 0:gq]),
                    (wkv.at[layer, :, pl.ds(al(grp * gkv, gkv), gkv)], w_at.at[layer, rows, gq:gq + gkv]),
                )
                ssem, rsem = wa_s.at[layer], wa_r.at[layer]
            else:
                j = idx - 1
                cols = pl.ds(al(grp * gff + j * CW, CW), CW)
                pieces = (
                    (wg.at[layer, :, cols], w_ml.at[layer, j, rows, 0:CW]),
                    (wu.at[layer, :, cols], w_ml.at[layer, j, rows, CW:2 * CW]),
                )
                ssem, rsem = w_s.at[layer], w_r.at[layer, j]
            for src, dst in pieces:
                if to is None:
                    local(src, dst, rsem)
                else:
                    send(src, dst, ssem, rsem, to)

    for idx in range(3):
        issue_w(0, idx)

    swap_wait(x_in.at[0:blk], xs_s, xs_r)
    res[...] = x_in[...].astype(F32)

    wait(packs, ps_r)
    for b in range(4):
        ang = packs[b, :, 128:256].astype(F32) * freq_ref[0:1, :]
        cos_t[b * blk:(b + 1) * blk, :] = jnp.cos(ang)
        sin_t[b * blk:(b + 1) * blk, :] = jnp.sin(ang)

    def rope(v, rows):
        lo, hi = v[:, 0:128].astype(F32), v[:, 128:256].astype(F32)
        cs, sn = cos_t[rows, :], sin_t[rows, :]
        return jnp.concatenate([lo * cs - hi * sn, hi * cs + lo * sn], axis=1).astype(BF16)

    own_rows = pl.ds(al(c * half, half), half)
    far_rows = pl.ds(al((1 - c) * half, half), half)
    y_rows = pl.ds(al(y * tb2, tb2), tb2)

    def group_at(s):
        return ((x + NX - s) * (1 - c) + (x + s - 1) * c) % NX

    def layer_body(layer, carry):
        for g in range(NX):
            for j in range(nch):
                local(wd.at[layer, g * gff + j * CW:g * gff + (j + 1) * CW], wb.at[j, g * CW:(g + 1) * CW], wb_r.at[layer])
        local(wo.at[layer], wb.at[nch], wb_r.at[layer])

        r = res[...]
        ssum = jnp.sum(r * r, axis=1, keepdims=True)
        stat = jnp.broadcast_to(ssum, (tb2, 128)).T[0:8]
        stat_own[...] = stat
        for d in range(1, 2 * NX):
            q = (me_plane + d) % (2 * NX)
            send(stat_own, stat_in.at[layer, d - 1], st_s.at[layer], st_r.at[layer], dev(tb=q // 2, ta=q % 2))
        issue_w(layer, 3)
        wait(stat_in.at[layer], st_r.at[layer])
        total = stat
        for d in range(2 * NX - 1):
            total = total + stat_in[layer, d]
        mean = jnp.broadcast_to(total[0:1], (128, tb2)).T[:, 0:1] / (kw * 2 * NX)
        normed = (r * lax.rsqrt(mean + NORM_EPS) * gain_ref[layer]).astype(BF16)
        own_cols = pl.ds(al((2 + c) * kw, kw), kw)
        h_buf[y_rows, own_cols] = normed
        mine = h_buf.at[y_rows, own_cols]
        send(mine, h_buf.at[y_rows, pl.ds(al(c * kw, kw), kw)], h_s.at[layer], h_r.at[layer], dev(tb=right, ta=0))
        send(mine, h_buf.at[y_rows, pl.ds(al(c * kw, kw), kw)], h_s.at[layer], h_r.at[layer], dev(tb=left, ta=1))
        send(mine, mine, h_s.at[layer], h_r.at[layer], sib)
        for d in range(1, NY):
            send(mine, mine, y_s.at[layer], y_r.at[layer], dev(mp=(y + d) % NY))
        issue_w(layer, 4)
        wait(h_buf.at[0:3 * tb2, 0:kw], h_r.at[layer])
        near = h_buf.at[y_rows, 0:2 * kw]
        other = h_buf.at[y_rows, pl.ds(al((3 - c) * kw, kw), kw)]
        for d in range(1, NY):
            send(near, near, y_s.at[layer], y_r.at[layer], dev(mp=(y + d) % NY))
        for d in range(1, NY):
            send(other, other, y_s.at[layer], y_r.at[layer], dev(mp=(y + d) % NY))
        acc[...] = jnp.zeros_like(acc)
        wait(h_buf.at[0:3 * tb2, :], y_r.at[layer])

        def share(j, g):
            blkref = m_buf.at[j, c, g]
            send(blkref, blkref, d_s.at[layer], d_r.at[layer, j], sib)

        def stage_m_out(j, m):
            m_buf[j, c, group] = m
            blkref = m_buf.at[j, c, group]
            send(blkref, blkref, ring_s.at[layer], ring_r.at[layer, j, 0], ring)
            share(j, group)

        def stage_r(j, s):
            g = group_at(s)
            blkref = m_buf.at[j, c, g]
            wait(blkref, ring_r.at[layer, j, s - 1])
            if s < NX - 1:
                send(blkref, blkref, ring_s.at[layer], ring_r.at[layer, j, s], ring)
            share(j, g)

        def stage_d(j):
            wait(m_buf.at[j, 1 - c], d_r.at[layer, j])
            for hf in range(2):
                lhs = jnp.concatenate([m_buf[j, hf, g] for g in range(NX)], axis=1)
                acc[hf * half:(hf + 1) * half, :] += jnp.dot(lhs, wb[j], preferred_element_type=F32)

        def stage_p(j):
            wait(w_ml.at[layer, j], w_r.at[layer, j])
            for n in range(2):
                zs[j, :, n * CW:(n + 1) * CW] = jnp.dot(h_buf[...], w_ml[layer, j, :, n * CW:(n + 1) * CW], preferred_element_type=F32)
            send(zs.at[j, far_rows], zr.at[j], p_s.at[layer, j], p_r.at[layer, j], partner)

        def stage_m(j):
            wait(zr.at[j], p_r.at[layer, j])
            z = zs[j, own_rows, :] + zr[j]
            gate = z[:, 0:CW].astype(BF16).astype(F32)
            up = z[:, CW:2 * CW].astype(BF16).astype(F32)
            stage_m_out(j, (jax.nn.silu(gate) * up).astype(BF16))

        def attn_p():
            wait(w_at.at[layer], wa_r.at[layer])
            za[...] = jnp.dot(h_buf[...], w_at[layer], preferred_element_type=F32)
            send(za.at[far_rows], zar, p_s.at[layer, nch], p_r.at[layer, nch], partner)

        def attn_m():
            wait(zar, p_r.at[layer, nch])
            z = za[own_rows, :] + zar[...]
            q_buf[...] = z[:, 0:gq].astype(BF16)
            kv_buf[group] = z[:, gq:gq + gkv].astype(BF16)
            send(kv_buf.at[group], kv_buf.at[group], kv_s.at[layer], kv_r.at[layer, 0], ring)

        def attn_r(s):
            g = group_at(s)
            wait(kv_buf.at[g], kv_r.at[layer, s - 1])
            if s < NX - 1:
                send(kv_buf.at[g], kv_buf.at[g], kv_s.at[layer], kv_r.at[layer, s], ring)

        def attn_core():
            outs = []
            for b in range(4):
                rows = slice(b * blk, (b + 1) * blk)
                q = rope(q_buf[rows, :], rows)
                k = rope(jnp.concatenate([kv_buf[0, rows, :], kv_buf[1, rows, :]], axis=1), rows)
                v = jnp.concatenate([kv_buf[2, rows, :], kv_buf[3, rows, :]], axis=1)
                scores = lax.dot_general(q, k, (((1,), (1,)), ((), ())), preferred_element_type=F32) * (gq ** -0.5)
                scores = jnp.where(packs[b, :, 0:blk].astype(F32) > 0.5, scores, -1e30)
                ex = jnp.exp(scores - jnp.max(scores, axis=1, keepdims=True))
                prob = (ex / jnp.sum(ex, axis=1, keepdims=True)).astype(BF16)
                outs.append(jnp.dot(prob, v, preferred_element_type=F32).astype(BF16))
            stage_m_out(nch, jnp.concatenate(outs, axis=0))

        for t in range(nch + 5):
            if 0 <= t - 4 < nch:
                stage_r(t - 4, 3)
            if t == 7:
                stage_r(nch, 3)
            if 0 <= t - 3 < nch:
                stage_r(t - 3, 2)
            if t == 6:
                stage_r(nch, 2)
            if 0 <= t - 2 < nch:
                stage_r(t - 2, 1)
            if t == 5:
                stage_r(nch, 1)
            if t == 0:
                attn_p()
            if t in (2, 3, 4):
                attn_r(t - 1)
            if 0 <= t - 1 < nch:
                stage_m(t - 1)
            if t == 1:
                attn_m()
            if t < nch:
                stage_p(t)
            if t in (0, 1):
                issue_w(layer, 5 + t)
            if t in (7, 8, 9):
                @pl.when(layer < layers - 1)
                def _():
                    issue_w(layer + 1, t - 7)
            if t == 4:
                attn_core()
            if t == 5:
                wait(wb, wb_r.at[layer])
            if 0 <= t - 5 < nch:
                stage_d(t - 5)
            if t == 8:
                stage_d(nch)

        for d in range(1, NY):
            to = (y + d) % NY
            send(acc.at[pl.ds(al(to * tb2, tb2), tb2)], rs_in.at[d - 1], rs_s.at[layer], rs_r.at[layer], dev(mp=to))
        wait(rs_in, rs_r.at[layer])
        res[...] = res[...] + (acc[y_rows, :] + rs_in[0] + rs_in[1] + rs_in[2])

        wait(stat_in.at[layer], st_s.at[layer])
        wait(h_buf.at[0:3 * tb2, 0:kw], h_s.at[layer])
        wait(h_buf.at[0:3 * tb2, :], y_s.at[layer])
        for j in range(nch):
            wait(zr.at[j], p_s.at[layer, j])
        wait(zar, p_s.at[layer, nch])
        wait(kv_buf.at[0:NX - 1], kv_s.at[layer])
        wait(m_buf.at[:, 0, 0:NX - 1], ring_s.at[layer])
        wait(m_buf.at[:, 0], d_s.at[layer])
        wait(rs_in, rs_s.at[layer])
        wait(w_at.at[layer, 0:3 * kw], wa_s.at[layer])
        wait(w_ml.at[layer, :, 0:3 * kw], w_s.at[layer])
        return carry

    lax.fori_loop(0, layers, layer_body, 0)

    swap_start(lambda t: res.at[t * blk:(t + 1) * blk], f_in.at[:, pl.ds(al(c * kw, kw), kw)], f_s, f_r)
    swap_wait(res.at[0:blk], f_s, f_r)
    out_ref[...] = f_in[...]

    @pl.when(jnp.logical_not(pack_own))
    def _():
        wait(pack_ref, ps_s.at[0])

    for d in range(1, NX):
        wait(pack_ref, ps_s.at[d])


def solution(mesh):
    def device_body(x_loc, seg_ids, pos_ids, w_q, w_k, w_v, w_gate, w_up, w_out, w_down, gain):
        blk, width_loc = x_loc.shape
        layers, kw, _ = w_q.shape
        head_dim = w_k.shape[-1]
        gq = w_q.shape[-1] // NX
        gff = w_gate.shape[-1] // NX
        gkv = 2 * head_dim // NX
        nch = gff // CW
        tok, half, tb2 = 8 * blk, 4 * blk, 2 * blk
        kg = 4 * kw
        allowed = (seg_ids[:, None] == seg_ids[None, :]) & (pos_ids[None, :] <= pos_ids[:, None])
        pack = jnp.concatenate([
            jnp.pad(allowed.astype(BF16), ((0, 0), (0, 128 - blk))),
            jnp.broadcast_to(pos_ids.astype(BF16)[:, None], (blk, 128)),
        ], axis=1)
        half_dim = head_dim // 2
        freq = ROPE_BASE ** (-(jnp.arange(half_dim, dtype=F32) * 2.0) / head_dim)
        freq = jnp.broadcast_to(freq[None], (8, half_dim))
        place = 2 * lax.axis_index("tb") + lax.axis_index("ta")
        gain_loc = lax.dynamic_slice(gain, (0, place * kw), (layers, kw)).astype(F32)[:, None, :]
        wkv = jnp.concatenate([w_k, w_v], axis=-1)
        hbm = pl.BlockSpec(memory_space=pl.ANY)
        vmem = pl.BlockSpec(memory_space=pltpu.VMEM)
        dma = pltpu.SemaphoreType.DMA
        return pl.pallas_call(
            functools.partial(kernel, (layers, blk, kw, gq, gkv, gff)),
            out_shape=jax.ShapeDtypeStruct((blk, width_loc), F32),
            in_specs=[vmem] * 4 + [hbm] * 6,
            out_specs=vmem,
            scratch_shapes=[
                pltpu.VMEM((layers, kg, gq + gkv), BF16),
                pltpu.VMEM((layers, nch, kg, 2 * CW), BF16),
                pltpu.VMEM((nch + 1, NX * CW, kw), BF16),
                pltpu.VMEM((nch, tok, 2 * CW), F32),
                pltpu.VMEM((nch, half, 2 * CW), F32),
                pltpu.VMEM((tok, gq + gkv), F32),
                pltpu.VMEM((half, gq + gkv), F32),
                pltpu.VMEM((nch + 1, 2, NX, half, CW), BF16),
                pltpu.VMEM((tok, kg), BF16),
                pltpu.VMEM((tok, kw), F32),
                pltpu.VMEM((tb2, kw), F32),
                pltpu.VMEM((NX, half, gkv), BF16),
                pltpu.VMEM((half, gq), BF16),
                pltpu.VMEM((half, half_dim), F32),
                pltpu.VMEM((half, half_dim), F32),
                pltpu.VMEM((4, blk, 256), BF16),
                pltpu.VMEM((8, tb2), F32),
                pltpu.VMEM((layers, 2 * NX - 1, 8, tb2), F32),
                pltpu.VMEM((NY - 1, tb2, kw), F32),
                pltpu.VMEM((tb2, kw), BF16),
                pltpu.VMEM((blk, width_loc), F32),
                dma((2,)), dma((2,)), dma((NX,)), dma(()),
                dma((layers,)), dma((layers,)), dma((layers, nch)), dma((layers,)), dma((layers,)),
                dma((layers, nch + 1)), dma((layers, nch + 1)),
                dma((layers,)), dma((layers, nch + 1, NX - 1)), dma((layers,)), dma((layers, nch + 1)),
                dma((layers,)), dma((layers, NX - 1)), dma((layers,)), dma((layers,)),
                dma((layers,)), dma((layers,)), dma((layers,)), dma((layers,)), dma((layers,)), dma((layers,)),
                dma((2,)), dma((2,)),
            ],
            compiler_params=pltpu.CompilerParams(collective_id=0, has_side_effects=True, vmem_limit_bytes=60 * 1024 * 1024),
        )(x_loc, pack, freq, gain_loc, w_q, wkv, w_gate, w_up, w_out, w_down)

    col_spec = P(None, PLANE_AXES, "mp")
    kv_spec = P(None, PLANE_AXES, None)
    row_spec = P(None, "mp", PLANE_AXES)
    return jax.shard_map(
        device_body,
        mesh=mesh,
        in_specs=(P(TOKEN_AXES, "mp"), P(TOKEN_AXES), P(TOKEN_AXES), col_spec, kv_spec, kv_spec, col_spec, col_spec, row_spec, row_spec, P(None, None)),
        out_specs=P(TOKEN_AXES, "mp"),
        check_vma=False,
    )
```

```python
import functools
import math

import jax
import jax.numpy as jnp
from jax import lax
from jax.experimental import pallas as pl
from jax.experimental.pallas import tpu as pltpu
from jax.sharding import PartitionSpec as P

ROPE_BASE = 10000.0
NORM_EPS = 1e-6
TOKEN_AXES = ("rep", "tb", "ta")
PLANE_AXES = ("tb", "ta")
MESH = pl.DeviceIdType.MESH
BF16, F32 = jnp.bfloat16, jnp.float32
NX, NY = 4, 4
CW = 256


def al(index, unit):
    return pl.multiple_of(index, unit)


def kernel(dims, x_ref, seg_ref, pos_ref, gain_ref, wq, wk, wv, wg, wu, wo, wd, out_ref,
           w_at, w_ml, wb, zs, zr, za, zar, zkv, m_buf, h_buf, acc, res, kv_buf, q_buf, cos_t, sin_t, packs,
           stat_own, stat_in, rs_in, rl_in, x_in, f_in, pack_ref, ids_t,
           xs_s, xs_r, ps_s, ps_r, w_s, wa_s, w_r, wa_r, wb_r, p_s, p_r, ring_s, ring_r, d_s, d_r,
           kv_s, kv_r, h_s, h_r, y_s, y_r, y0_s, y0_r, sb_s, sb_r, st_s, st_r, rs_s, rs_r, rl_s, rl_r, f_s, f_r, kvx_s, kvx_r, kvy_s, kvy_r, kvp_s, kvp_r, kvz_s, kvz_r):
    layers, blk, kw, gq, gkv, gff = dims
    nch = gff // CW
    tok = 8 * blk
    half = tok // 2
    tb2 = 2 * blk
    x, c, y = lax.axis_index("tb"), lax.axis_index("ta"), lax.axis_index("mp")
    right, left = (x + 1) % NX, (x + NX - 1) % NX
    nxt = right * (1 - c) + left * c
    prv = left * (1 - c) + right * c
    group = (x + NX - c) % NX

    def dev(tb=None, ta=None, mp=None):
        return {"tb": x if tb is None else tb, "ta": c if ta is None else ta, "mp": y if mp is None else mp}

    sib = dev(ta=1 - c)
    ring = dev(tb=nxt)
    partner = dev(tb=nxt, ta=1 - c)

    def send(src, dst, ssem, rsem, to):
        pltpu.make_async_remote_copy(src_ref=src, dst_ref=dst, send_sem=ssem, recv_sem=rsem, device_id=to, device_id_type=MESH).start()

    def local(src, dst, sem):
        pltpu.make_async_copy(src, dst, sem).start()

    def wait(ref, sem):
        pltpu.make_async_copy(ref, ref, sem).wait()

    me_plane = 2 * x + c
    barrier = pltpu.get_barrier_semaphore()
    for d in range(1, 2 * NX):
        q = (me_plane + d) % (2 * NX)
        pl.semaphore_signal(barrier, inc=1, device_id=dev(tb=q // 2, ta=q % 2), device_id_type=MESH)
    for d in range(1, NY):
        pl.semaphore_signal(barrier, inc=1, device_id=dev(mp=(y + d) % NY), device_id_type=MESH)

    peers = 2 * NX - 1 + NY - 1

    @pl.when(x != y)
    def _():
        for t in range(2):
            pl.semaphore_signal(barrier, inc=1, device_id=dev(tb=y, ta=t, mp=x), device_id_type=MESH)
        pl.semaphore_wait(barrier, peers + 2)

    @pl.when(x == y)
    def _():
        pl.semaphore_wait(barrier, peers)

    def swap_start(src_of, dst, ssem, rsem):
        for t in range(2):
            own = jnp.logical_and(x == y, c == t)

            @pl.when(own)
            def _():
                local(src_of(t), dst, rsem.at[c])

            @pl.when(jnp.logical_not(own))
            def _():
                send(src_of(t), dst, ssem.at[t], rsem.at[c], dev(tb=y, ta=t, mp=x))

    def swap_wait(part, ssem, rsem):
        for t in range(2):
            wait(part, rsem.at[t])

            @pl.when(jnp.logical_not(jnp.logical_and(x == y, c == t)))
            def _():
                wait(part, ssem.at[t])

    swap_start(lambda t: x_ref.at[:, t * kw:(t + 1) * kw], x_in.at[pl.ds(al(c * blk, blk), blk)], xs_s, xs_r)

    qr = kw // NY

    def kv_quarter(slot):
        return pl.ds(al(slot * kw + y * qr, qr), qr)

    def kv_spread(layer):
        wait(w_at.at[layer, 0:2 * qr, gq:gq + gkv], kvx_r.at[layer])
        for d in range(1, NY):
            for slot in range(2):
                piece = w_at.at[layer, kv_quarter(slot), gq:gq + gkv]
                send(piece, piece, kvy_s.at[layer], kvy_r.at[layer], dev(mp=(y + d) % NY))

    def issue_w(layer, idx, part):
        if part == 0:
            targets = (((prv + NX + c - 1) % NX, c, dev(tb=prv, ta=1 - c)), ((x + 3 + c) % NX, 2 + c, sib), (group, 2 + c, None))
        else:
            targets = (((nxt + NX - c) % NX, c, ring),)
        for grp, slot, to in targets:
            rows = pl.ds(al(slot * kw, kw), kw)

            def put(src, dst, ssem, rsem):
                if to is None:
                    local(src, dst, rsem)
                else:
                    send(src, dst, ssem, rsem, to)

            if idx == 0:
                ssem, rsem = wa_s.at[layer], wa_r.at[layer]
                put(wq.at[layer, :, pl.ds(al(grp * gq, gq), gq)], w_at.at[layer, rows, 0:gq], ssem, rsem)
                kv_cols = pl.ds(al((grp % 2) * gkv, gkv), gkv)
                if to is None or to is sib:
                    kv_src, kv_rows, kv_sems = slice(None), rows, (ssem, rsem)
                else:
                    kv_src, kv_rows, kv_sems = pl.ds(al(y * qr, qr), qr), kv_quarter(slot), (kvx_s.at[layer], kvx_r.at[layer])
                kv_dst = w_at.at[layer, kv_rows, gq:gq + gkv]

                @pl.when(grp < 2)
                def _():
                    put(wk.at[layer, kv_src, kv_cols], kv_dst, *kv_sems)

                @pl.when(grp >= 2)
                def _():
                    put(wv.at[layer, kv_src, kv_cols], kv_dst, *kv_sems)
            else:
                j = idx - 1
                cols = pl.ds(al(grp * gff + j * CW, CW), CW)
                ssem, rsem = w_s.at[layer], w_r.at[layer, j]
                put(wg.at[layer, :, cols], w_ml.at[layer, j, rows, 0:CW], ssem, rsem)
                put(wu.at[layer, :, cols], w_ml.at[layer, j, rows, CW:2 * CW], ssem, rsem)

    issue_w(0, 0, 0)
    issue_w(0, 0, 1)

    ids_t[...] = jnp.zeros_like(ids_t)
    ids_t[:, 0:blk] = jnp.broadcast_to(seg_ref[...], (128, blk))
    seg_rows, seg_cols = ids_t[0:blk, 0:blk], ids_t[...].T[0:blk, 0:blk]
    ids_t[:, 0:blk] = jnp.broadcast_to(pos_ref[...], (128, blk))
    pos_rows, pos_cols = ids_t[0:blk, 0:blk], ids_t[...].T[0:blk]
    allowed = (seg_rows == seg_cols) & (pos_rows <= pos_cols[:, 0:blk])
    pack_ref[...] = jnp.zeros_like(pack_ref)
    pack_ref[:, 0:blk] = jnp.where(allowed, 1.0, 0.0).astype(BF16)
    pack_ref[:, 128:256] = pos_cols.astype(F32).astype(BF16)

    pack_slot = (x % 2) * 2 + c
    pack_core = x // 2
    pack_own = c == pack_core

    @pl.when(pack_own)
    def _():
        local(pack_ref, packs.at[pack_slot], ps_r)

    @pl.when(jnp.logical_not(pack_own))
    def _():
        send(pack_ref, packs.at[pack_slot], ps_s.at[0], ps_r, dev(ta=pack_core))

    for d in range(1, NX):
        send(pack_ref, packs.at[pack_slot], ps_s.at[d], ps_r, dev(tb=(x + d) % NX, ta=pack_core))

    for idx in (1, 2):
        issue_w(0, idx, 0)
        issue_w(0, idx, 1)
    swap_wait(x_in.at[0:blk], xs_s, xs_r)
    res[...] = x_in[...].astype(F32)

    def tables():
        wait(packs, ps_r)
        lane = lax.broadcasted_iota(jnp.int32, (8, gq // 2), 1).astype(F32)
        freq = jnp.exp(lane * (-2.0 * math.log(ROPE_BASE) / gq))[0:1]
        for b in range(4):
            ang = packs[b, :, 128:256].astype(F32) * freq
            cos_t[b * blk:(b + 1) * blk, :] = jnp.cos(ang)
            sin_t[b * blk:(b + 1) * blk, :] = jnp.sin(ang)

    def rope(v, rows):
        lo, hi = v[:, 0:128].astype(F32), v[:, 128:256].astype(F32)
        cs, sn = cos_t[rows, :], sin_t[rows, :]
        return jnp.concatenate([lo * cs - hi * sn, hi * cs + lo * sn], axis=1).astype(BF16)

    own_rows = pl.ds(al(c * half, half), half)
    far_rows = pl.ds(al((1 - c) * half, half), half)
    y_rows = pl.ds(al(y * tb2, tb2), tb2)

    def group_at(s):
        return ((x + NX - s) * (1 - c) + (x + s - 1) * c) % NX

    def issue_all(layer, units):
        for idx, part in units:
            issue_w(layer, idx, part)

    def layer_body(layer, carry):
        for g in range(NX):
            for j in range(nch):
                local(wd.at[layer, g * gff + j * CW:g * gff + (j + 1) * CW], wb.at[j, g * CW:(g + 1) * CW], wb_r.at[layer])
        local(wo.at[layer], wb.at[nch], wb_r.at[layer])

        r = res[...]
        ssum = jnp.sum(r * r, axis=1, keepdims=True)
        stat = jnp.broadcast_to(ssum, (tb2, 128)).T[0:8]
        stat_own[...] = stat
        for d in range(1, 2 * NX):
            q = (me_plane + d) % (2 * NX)
            send(stat_own, stat_in.at[layer, d - 1], st_s.at[layer], st_r.at[layer], dev(tb=q // 2, ta=q % 2))
        issue_all(layer, ((3, 0), (3, 1)))
        wait(stat_in.at[layer], st_r.at[layer])
        total = stat
        for d in range(2 * NX - 1):
            total = total + stat_in[layer, d]
        mean = jnp.broadcast_to(total[0:1], (128, tb2)).T[:, 0:1] / (kw * 2 * NX)
        gains = gain_ref[:, pl.ds(al(me_plane * kw, 128), kw)].astype(F32)
        gain = jnp.where(layer == 0, gains[0:1], gains[1:2])
        normed = (r * lax.rsqrt(mean + NORM_EPS) * gain).astype(BF16)
        own_cols = pl.ds(al((2 + c) * kw, kw), kw)
        h_buf[y_rows, own_cols] = normed
        mine = h_buf.at[y_rows, own_cols]
        far = h_buf.at[y_rows, pl.ds(al(c * kw, kw), kw)]
        send(mine, far, h_s.at[layer], h_r.at[layer], dev(tb=right, ta=0))
        send(mine, far, h_s.at[layer], h_r.at[layer], dev(tb=left, ta=1))
        for d in range(1, NY):
            send(mine, mine, y0_s.at[layer], y0_r.at[layer], dev(mp=(y + d) % NY))
        issue_all(layer, ((4, 0), (4, 1), (5, 0)))
        acc[...] = jnp.zeros_like(acc)
        wait(h_buf.at[y_rows, 0:2 * kw], h_r.at[layer])
        near = h_buf.at[y_rows, 0:2 * kw]
        for d in range(1, NY):
            send(near, near, y_s.at[layer], y_r.at[layer], dev(mp=(y + d) % NY))
        kv_spread(layer)
        wait(h_buf.at[0:3 * tb2, 0:kw], y0_r.at[layer])
        send(h_buf.at[:, own_cols], h_buf.at[:, own_cols], sb_s.at[layer], sb_r.at[layer], sib)
        wait(h_buf.at[0:3 * tb2, 0:2 * kw], y_r.at[layer])
        wait(h_buf.at[:, 0:kw], sb_r.at[layer])

        def share(j, g):
            blkref = m_buf.at[j, c, g]
            send(blkref, blkref, d_s.at[layer], d_r.at[layer, j], sib)

        def stage_m_out(j, m):
            m_buf[j, c, group] = m
            blkref = m_buf.at[j, c, group]
            send(blkref, blkref, ring_s.at[layer], ring_r.at[layer, j, 0], ring)
            share(j, group)

        def stage_r(j, s):
            g = group_at(s)
            blkref = m_buf.at[j, c, g]
            wait(blkref, ring_r.at[layer, j, s - 1])
            if s < NX - 1:
                send(blkref, blkref, ring_s.at[layer], ring_r.at[layer, j, s], ring)
            share(j, g)

        def stage_d(j):
            wait(m_buf.at[j, 1 - c], d_r.at[layer, j])
            for hf in range(2):
                lhs = jnp.concatenate([m_buf[j, hf, g] for g in range(NX)], axis=1)
                acc[hf * half:(hf + 1) * half, :] += jnp.dot(lhs, wb[j], preferred_element_type=F32)

        def stage_p(j):
            wait(w_ml.at[layer, j], w_r.at[layer, j])
            for n in range(2):
                zs[j, :, n * CW:(n + 1) * CW] = jnp.dot(h_buf[...], w_ml[layer, j, :, n * CW:(n + 1) * CW], preferred_element_type=F32)
            send(zs.at[j, far_rows], zr.at[j], p_s.at[layer, j], p_r.at[layer, j], partner)

        def stage_m(j):
            wait(zr.at[j], p_r.at[layer, j])
            z = zs[j, own_rows, :] + zr[j]
            gate = z[:, 0:CW].astype(BF16).astype(F32)
            up = z[:, CW:2 * CW].astype(BF16).astype(F32)
            stage_m_out(j, (jax.nn.silu(gate) * up).astype(BF16))

        def attn_p():
            wait(w_at.at[layer, 0:(4 * kw * gq + 2 * kw * gkv) // (gq + gkv)], wa_r.at[layer])
            wait(w_at.at[layer, 0:6 * qr, gq:gq + gkv], kvy_r.at[layer])
            za[...] = jnp.dot(h_buf[...], w_at[layer], preferred_element_type=F32)
            send(za.at[far_rows, 0:gq], zar, p_s.at[layer, nch], p_r.at[layer, nch], partner)
            send(za.at[pl.ds(al((1 - c) * half + y * blk, blk), blk), gq:gq + gkv], zkv, kvp_s.at[layer], kvp_r.at[layer], partner)

        yb = pl.ds(al(y * blk, blk), blk)

        def attn_m():
            wait(zkv, kvp_r.at[layer])
            kv_buf[group, yb, :] = (za[pl.ds(al(c * half + y * blk, blk), blk), gq:gq + gkv] + zkv[...]).astype(BF16)
            send(kv_buf.at[group, yb], kv_buf.at[group, yb], kv_s.at[layer], kv_r.at[layer, 0], ring)
            wait(zar, p_r.at[layer, nch])
            q_buf[...] = (za[own_rows, 0:gq] + zar[...]).astype(BF16)

        def attn_r(s):
            g = group_at(s)
            blkref = kv_buf.at[g, yb]
            wait(blkref, kv_r.at[layer, s - 1])
            if s < NX - 1:
                send(blkref, blkref, kv_s.at[layer], kv_r.at[layer, s], ring)
            else:
                for d in range(1, NY):
                    send(kv_buf.at[:, yb], kv_buf.at[:, yb], kvz_s.at[layer], kvz_r.at[layer], dev(mp=(y + d) % NY))

        def attn_core():
            wait(kv_buf.at[0:NX - 1], kvz_r.at[layer])
            outs = []
            for b in range(4):
                rows = slice(b * blk, (b + 1) * blk)
                q = rope(q_buf[rows, :], rows)
                k = rope(jnp.concatenate([kv_buf[0, rows, :], kv_buf[1, rows, :]], axis=1), rows)
                v = jnp.concatenate([kv_buf[2, rows, :], kv_buf[3, rows, :]], axis=1)
                scores = lax.dot_general(q, k, (((1,), (1,)), ((), ())), preferred_element_type=F32) * (gq ** -0.5)
                scores = jnp.where(packs[b, :, 0:blk].astype(F32) > 0.5, scores, -1e30)
                ex = jnp.exp(scores - jnp.max(scores, axis=1, keepdims=True))
                prob = (ex / jnp.sum(ex, axis=1, keepdims=True)).astype(BF16)
                outs.append(jnp.dot(prob, v, preferred_element_type=F32).astype(BF16))
            stage_m_out(nch, jnp.concatenate(outs, axis=0))

        last = nch - 1
        issue_all(layer, ((5, 1), (6, 0), (6, 1)))
        attn_p()
        for j in range(nch):
            stage_p(j)
        pl.when(layer == 0)(tables)
        attn_m()
        for j in range(nch):
            stage_m(j)
        wait(h_buf.at[:, 0:kw], sb_s.at[layer])
        wait(wb, wb_r.at[layer])
        attn_r(1)
        stage_r(0, 1)
        stage_r(1, 1)
        attn_r(2)
        stage_r(2, 1)
        stage_r(3, 1)
        attn_r(3)
        for j in range(4, nch):
            stage_r(j, 1)
        attn_core()
        for j in range(3):
            stage_r(j, 2)
        stage_r(nch, 1)
        for j in range(3, nch):
            stage_r(j, 2)
        stage_r(0, 3)
        stage_r(nch, 2)
        stage_r(1, 3)

        @pl.when(layer < layers - 1)
        def _():
            issue_all(layer + 1, ((0, 0), (0, 1), (1, 0), (1, 1), (2, 0), (2, 1)))

        stage_d(0)
        for j in range(2, nch):
            stage_r(j, 3)
            stage_d(j - 1)
        stage_r(nch, 3)
        stage_d(last)
        stage_d(nch)

        up, dn, op = (y + 1) % NY, (y + NY - 1) % NY, (y + 2) % NY

        def part(block, second):
            return pl.ds(al(block * tb2 + second * blk, blk), blk)

        def to_y(rows, dst, rsem, to):
            send(acc.at[rows], dst, rs_s.at[layer], rsem, dev(mp=to))

        send(acc.at[part(op, 0)], rl_in.at[0], rl_s.at[layer, 0], rl_r.at[layer, 0], dev(mp=up))
        send(acc.at[part(op, 1)], rl_in.at[1], rl_s.at[layer, 1], rl_r.at[layer, 1], dev(mp=dn))
        wait(rl_in.at[0], rl_s.at[layer, 0])
        wait(rl_in.at[1], rl_s.at[layer, 1])
        to_y(part(up, 1), rs_in.at[0, blk:tb2], rs_r.at[layer], up)
        to_y(part(dn, 0), rs_in.at[1, 0:blk], rs_r.at[layer], dn)
        wait(rl_in.at[0], rl_r.at[layer, 0])
        acc[part(up, 0), :] += rl_in[0]
        to_y(part(up, 0), rs_in.at[0, 0:blk], rs_r.at[layer], up)
        wait(rl_in.at[1], rl_r.at[layer, 1])
        acc[part(dn, 1), :] += rl_in[1]
        to_y(part(dn, 1), rs_in.at[1, blk:tb2], rs_r.at[layer], dn)
        wait(rs_in, rs_r.at[layer])
        res[...] = res[...] + (acc[y_rows, :] + rs_in[0] + rs_in[1])

        wait(stat_in.at[layer], st_s.at[layer])
        wait(h_buf.at[0:tb2, 0:2 * kw], h_s.at[layer])
        wait(h_buf.at[0:3 * tb2, 0:kw], y0_s.at[layer])
        wait(h_buf.at[0:3 * tb2, 0:2 * kw], y_s.at[layer])
        for j in range(nch):
            wait(zr.at[j], p_s.at[layer, j])
        wait(zar, p_s.at[layer, nch])
        wait(kv_buf.at[0, 0:3 * blk], kv_s.at[layer])
        wait(kv_buf.at[0:NX - 1], kvz_s.at[layer])
        wait(zkv, kvp_s.at[layer])
        wait(w_at.at[layer, 0:2 * qr, gq:gq + gkv], kvx_s.at[layer])
        wait(w_at.at[layer, 0:6 * qr, gq:gq + gkv], kvy_s.at[layer])
        wait(m_buf.at[:, 0, 0:NX - 1], ring_s.at[layer])
        wait(m_buf.at[:, 0], d_s.at[layer])
        wait(acc.at[0:4 * blk], rs_s.at[layer])
        wait(w_at.at[layer, 0:(3 * kw * gq + kw * gkv) // (gq + gkv)], wa_s.at[layer])
        wait(w_ml.at[layer, :, 0:3 * kw], w_s.at[layer])
        return carry

    lax.fori_loop(0, layers, layer_body, 0)

    swap_start(lambda t: res.at[t * blk:(t + 1) * blk], f_in.at[:, pl.ds(al(c * kw, kw), kw)], f_s, f_r)
    swap_wait(res.at[0:blk], f_s, f_r)
    out_ref[...] = f_in[...]

    @pl.when(jnp.logical_not(pack_own))
    def _():
        wait(pack_ref, ps_s.at[0])

    for d in range(1, NX):
        wait(pack_ref, ps_s.at[d])


def solution(mesh):
    def device_body(x_loc, seg_ids, pos_ids, w_q, w_k, w_v, w_gate, w_up, w_out, w_down, gain):
        blk, width_loc = x_loc.shape
        layers, kw, _ = w_q.shape
        head_dim = w_k.shape[-1]
        gq = w_q.shape[-1] // NX
        gff = w_gate.shape[-1] // NX
        gkv = 2 * head_dim // NX
        nch = gff // CW
        tok, half, tb2 = 8 * blk, 4 * blk, 2 * blk
        kg = 4 * kw
        half_dim = head_dim // 2
        hbm = pl.BlockSpec(memory_space=pl.ANY)
        vmem = pl.BlockSpec(memory_space=pltpu.VMEM)
        dma = pltpu.SemaphoreType.DMA
        return pl.pallas_call(
            functools.partial(kernel, (layers, blk, kw, gq, gkv, gff)),
            out_shape=jax.ShapeDtypeStruct((blk, width_loc), F32),
            in_specs=[vmem] * 4 + [hbm] * 7,
            out_specs=vmem,
            scratch_shapes=[
                pltpu.VMEM((layers, kg, gq + gkv), BF16),
                pltpu.VMEM((layers, nch, kg, 2 * CW), BF16),
                pltpu.VMEM((nch + 1, NX * CW, kw), BF16),
                pltpu.VMEM((nch, tok, 2 * CW), F32),
                pltpu.VMEM((nch, half, 2 * CW), F32),
                pltpu.VMEM((tok, gq + gkv), F32),
                pltpu.VMEM((half, gq), F32),
                pltpu.VMEM((blk, gkv), F32),
                pltpu.VMEM((nch + 1, 2, NX, half, CW), BF16),
                pltpu.VMEM((tok, kg), BF16),
                pltpu.VMEM((tok, kw), F32),
                pltpu.VMEM((tb2, kw), F32),
                pltpu.VMEM((NX, half, gkv), BF16),
                pltpu.VMEM((half, gq), BF16),
                pltpu.VMEM((half, half_dim), F32),
                pltpu.VMEM((half, half_dim), F32),
                pltpu.VMEM((4, blk, 256), BF16),
                pltpu.VMEM((8, tb2), F32),
                pltpu.VMEM((layers, 2 * NX - 1, 8, tb2), F32),
                pltpu.VMEM((2, tb2, kw), F32),
                pltpu.VMEM((2, blk, kw), F32),
                pltpu.VMEM((tb2, kw), BF16),
                pltpu.VMEM((blk, width_loc), F32),
                pltpu.VMEM((blk, 256), BF16),
                pltpu.VMEM((128, 128), jnp.int32),
                dma((2,)), dma((2,)), dma((NX,)), dma(()),
                dma((layers,)), dma((layers,)), dma((layers, nch)), dma((layers,)), dma((layers,)),
                dma((layers, nch + 1)), dma((layers, nch + 1)),
                dma((layers,)), dma((layers, nch + 1, NX - 1)), dma((layers,)), dma((layers, nch + 1)),
                dma((layers,)), dma((layers, NX - 1)), dma((layers,)), dma((layers,)),
                dma((layers,)), dma((layers,)), dma((layers,)), dma((layers,)), dma((layers,)), dma((layers,)),
                dma((layers,)), dma((layers,)), dma((layers,)), dma((layers,)), dma((layers, 2)), dma((layers, 2)),
                dma((2,)), dma((2,)),
            ] + [dma((layers,))] * 8,
            compiler_params=pltpu.CompilerParams(collective_id=0, has_side_effects=True, vmem_limit_bytes=60 * 1024 * 1024),
        )(x_loc, seg_ids[None], pos_ids[None], gain, w_q, w_k, w_v, w_gate, w_up, w_out, w_down)

    col_spec = P(None, PLANE_AXES, "mp")
    kv_spec = P(None, PLANE_AXES, None)
    row_spec = P(None, "mp", PLANE_AXES)
    return jax.shard_map(
        device_body,
        mesh=mesh,
        in_specs=(P(TOKEN_AXES, "mp"), P(TOKEN_AXES), P(TOKEN_AXES), col_spec, kv_spec, kv_spec, col_spec, col_spec, row_spec, row_spec, P(None, None)),
        out_specs=P(TOKEN_AXES, "mp"),
        check_vma=False,
    )
```

```python
import functools
import math

import jax
import jax.numpy as jnp
from jax import lax
from jax.experimental import pallas as pl
from jax.experimental.pallas import tpu as pltpu
from jax.sharding import PartitionSpec as P

ROPE_BASE = 10000.0
NORM_EPS = 1e-6
TOKEN_AXES = ("rep", "tb", "ta")
PLANE_AXES = ("tb", "ta")
MESH = pl.DeviceIdType.MESH
BF16, F32 = jnp.bfloat16, jnp.float32
NX, NY = 4, 4
CW = 256


def al(index, unit):
    return pl.multiple_of(index, unit)


def kernel(dims, x_ref, seg_ref, pos_ref, gain_ref, wq, wk, wv, wg, wu, wo, wd, out_ref,
           w_at, w_ml, wb, zs, zr, za, zar, zkv, m_buf, h_buf, acc, res, kv_buf, q_buf, cos_t, sin_t, packs,
           stat_own, stat_in, rs_in, rl_in, x_in, f_in, pack_ref, ids_t,
           xs_s, xs_r, ps_s, ps_r, w_s, wa_s, w_r, wa_r, wb_r, p_s, p_r, ring_s, ring_r, d_s, d_r,
           kv_s, kv_r, h_s, h_r, y_s, y_r, y0_s, y0_r, sb_s, sb_r, st_s, st_r, rs_s, rs_r, rl_s, rl_r, f_s, f_r, kvx_s, kvx_r, kvy_s, kvy_r, kvp_s, kvp_r, kvz_s, kvz_r):
    layers, blk, kw, gq, gkv, gff = dims
    nch = gff // CW
    tok = 8 * blk
    half = tok // 2
    tb2 = 2 * blk
    x, c, y = lax.axis_index("tb"), lax.axis_index("ta"), lax.axis_index("mp")
    right, left = (x + 1) % NX, (x + NX - 1) % NX
    nxt = right * (1 - c) + left * c
    prv = left * (1 - c) + right * c
    group = (x + NX - c) % NX

    def dev(tb=None, ta=None, mp=None):
        return {"tb": x if tb is None else tb, "ta": c if ta is None else ta, "mp": y if mp is None else mp}

    sib = dev(ta=1 - c)
    ring = dev(tb=nxt)
    partner = dev(tb=nxt, ta=1 - c)

    def send(src, dst, ssem, rsem, to):
        pltpu.make_async_remote_copy(src_ref=src, dst_ref=dst, send_sem=ssem, recv_sem=rsem, device_id=to, device_id_type=MESH).start()

    def local(src, dst, sem):
        pltpu.make_async_copy(src, dst, sem).start()

    def wait(ref, sem):
        pltpu.make_async_copy(ref, ref, sem).wait()

    me_plane = 2 * x + c
    barrier = pltpu.get_barrier_semaphore()
    for d in range(1, 2 * NX):
        q = (me_plane + d) % (2 * NX)
        pl.semaphore_signal(barrier, inc=1, device_id=dev(tb=q // 2, ta=q % 2), device_id_type=MESH)
    for d in range(1, NY):
        pl.semaphore_signal(barrier, inc=1, device_id=dev(mp=(y + d) % NY), device_id_type=MESH)

    peers = 2 * NX - 1 + NY - 1

    @pl.when(x != y)
    def _():
        for t in range(2):
            pl.semaphore_signal(barrier, inc=1, device_id=dev(tb=y, ta=t, mp=x), device_id_type=MESH)
        pl.semaphore_wait(barrier, peers + 2)

    @pl.when(x == y)
    def _():
        pl.semaphore_wait(barrier, peers)

    def swap_send(t, src, dst, ssem, rsem):
        own = jnp.logical_and(x == y, c == t)

        @pl.when(own)
        def _():
            local(src, dst, rsem.at[c])

        @pl.when(jnp.logical_not(own))
        def _():
            send(src, dst, ssem.at[t], rsem.at[c], dev(tb=y, ta=t, mp=x))

    def swap_start(src_of, dst, ssem, rsem):
        for t in range(2):
            swap_send(t, src_of(t), dst, ssem, rsem)

    def swap_wait(part, ssem, rsem):
        for t in range(2):
            wait(part, rsem.at[t])

            @pl.when(jnp.logical_not(jnp.logical_and(x == y, c == t)))
            def _():
                wait(part, ssem.at[t])

    swap_start(lambda t: x_ref.at[:, t * kw:(t + 1) * kw], x_in.at[pl.ds(al(c * blk, blk), blk)], xs_s, xs_r)

    qr = kw // NY

    def kv_quarter(slot):
        return pl.ds(al(slot * kw + y * qr, qr), qr)

    def kv_spread(layer):
        wait(w_at.at[layer, 0:2 * qr, gq:gq + gkv], kvx_r.at[layer])
        for d in range(1, NY):
            for slot in range(2):
                piece = w_at.at[layer, kv_quarter(slot), gq:gq + gkv]
                send(piece, piece, kvy_s.at[layer], kvy_r.at[layer], dev(mp=(y + d) % NY))

    def issue_w(layer, idx, part):
        if part == 0:
            targets = (((prv + NX + c - 1) % NX, c, dev(tb=prv, ta=1 - c)), ((x + 3 + c) % NX, 2 + c, sib), (group, 2 + c, None))
        else:
            targets = (((nxt + NX - c) % NX, c, ring),)
        for grp, slot, to in targets:
            rows = pl.ds(al(slot * kw, kw), kw)

            def put(src, dst, ssem, rsem):
                if to is None:
                    local(src, dst, rsem)
                else:
                    send(src, dst, ssem, rsem, to)

            if idx == 0:
                ssem, rsem = wa_s.at[layer], wa_r.at[layer]
                put(wq.at[layer, :, pl.ds(al(grp * gq, gq), gq)], w_at.at[layer, rows, 0:gq], ssem, rsem)
                kv_cols = pl.ds(al((grp % 2) * gkv, gkv), gkv)
                if to is None or to is sib:
                    kv_src, kv_rows, kv_sems = slice(None), rows, (ssem, rsem)
                else:
                    kv_src, kv_rows, kv_sems = pl.ds(al(y * qr, qr), qr), kv_quarter(slot), (kvx_s.at[layer], kvx_r.at[layer])
                kv_dst = w_at.at[layer, kv_rows, gq:gq + gkv]

                @pl.when(grp < 2)
                def _():
                    put(wk.at[layer, kv_src, kv_cols], kv_dst, *kv_sems)

                @pl.when(grp >= 2)
                def _():
                    put(wv.at[layer, kv_src, kv_cols], kv_dst, *kv_sems)
            else:
                j = idx - 1
                cols = pl.ds(al(grp * gff + j * CW, CW), CW)
                ssem, rsem = w_s.at[layer], w_r.at[layer, j]
                put(wg.at[layer, :, cols], w_ml.at[layer, j, rows, 0:CW], ssem, rsem)
                put(wu.at[layer, :, cols], w_ml.at[layer, j, rows, CW:2 * CW], ssem, rsem)

    issue_w(0, 0, 0)
    issue_w(0, 0, 1)

    ids_t[...] = jnp.zeros_like(ids_t)
    ids_t[:, 0:blk] = jnp.broadcast_to(seg_ref[...], (128, blk))
    seg_rows, seg_cols = ids_t[0:blk, 0:blk], ids_t[...].T[0:blk, 0:blk]
    ids_t[:, 0:blk] = jnp.broadcast_to(pos_ref[...], (128, blk))
    pos_rows, pos_cols = ids_t[0:blk, 0:blk], ids_t[...].T[0:blk]
    allowed = (seg_rows == seg_cols) & (pos_rows <= pos_cols[:, 0:blk])
    pack_ref[...] = jnp.zeros_like(pack_ref)
    pack_ref[:, 0:blk] = jnp.where(allowed, 1.0, 0.0).astype(BF16)
    pack_ref[:, 128:256] = pos_cols.astype(F32).astype(BF16)

    pack_slot = c * 2 + x % 2
    pack_core = x // 2
    pack_own = c == pack_core

    @pl.when(pack_own)
    def _():
        local(pack_ref, packs.at[pack_slot], ps_r)

    @pl.when(jnp.logical_not(pack_own))
    def _():
        send(pack_ref, packs.at[pack_slot], ps_s.at[0], ps_r, dev(ta=pack_core))

    for d in range(1, NX):
        send(pack_ref, packs.at[pack_slot], ps_s.at[d], ps_r, dev(tb=(x + d) % NX, ta=pack_core))

    for idx in (1, 2):
        issue_w(0, idx, 0)
        issue_w(0, idx, 1)
    swap_wait(x_in.at[0:blk], xs_s, xs_r)
    res[...] = x_in[...].astype(F32)

    def tables():
        wait(packs, ps_r)
        lane = lax.broadcasted_iota(jnp.int32, (8, gq // 2), 1).astype(F32)
        freq = jnp.exp(lane * (-2.0 * math.log(ROPE_BASE) / gq))[0:1]
        for b in range(4):
            ang = packs[b, :, 128:256].astype(F32) * freq
            cos_t[b * blk:(b + 1) * blk, :] = jnp.cos(ang)
            sin_t[b * blk:(b + 1) * blk, :] = jnp.sin(ang)

    def rope(v, rows):
        lo, hi = v[:, 0:128].astype(F32), v[:, 128:256].astype(F32)
        cs, sn = cos_t[rows, :], sin_t[rows, :]
        return jnp.concatenate([lo * cs - hi * sn, hi * cs + lo * sn], axis=1).astype(BF16)

    own_rows = pl.ds(al(c * half, half), half)
    far_rows = pl.ds(al((1 - c) * half, half), half)
    yh, yl = y // 2, y % 2
    sub = half // 2

    def sized(rows):
        return w_at.at[0, 0:rows]

    def hidden():
        return h_buf[...].reshape(tok, 4 * kw)

    def group_at(s):
        return ((x + NX - s) * (1 - c) + (x + s - 1) * c) % NX

    def group_back(s):
        return ((x + s) * (1 - c) + (x + 2 * NX - s - 1) * c) % NX

    back = dev(tb=prv)

    def issue_all(layer, units):
        for idx, part in units:
            issue_w(layer, idx, part)

    def layer_body(layer, carry):
        for g in range(NX):
            for j in range(nch):
                local(wd.at[layer, g * gff + j * CW:g * gff + (j + 1) * CW], wb.at[j, g * CW:(g + 1) * CW], wb_r.at[layer])
        local(wo.at[layer], wb.at[nch], wb_r.at[layer])

        r = res[...]
        ssum = jnp.sum(r * r, axis=1, keepdims=True)
        stat = jnp.broadcast_to(ssum, (tb2, 128)).T[0:8]
        stat_own[...] = stat
        for d in range(1, 2 * NX):
            q = (me_plane + d) % (2 * NX)
            send(stat_own, stat_in.at[layer, d - 1], st_s.at[layer], st_r.at[layer], dev(tb=q // 2, ta=q % 2))
        issue_all(layer, ((3, 0), (3, 1)))
        wait(stat_in.at[layer], st_r.at[layer])
        total = stat
        for d in range(2 * NX - 1):
            total = total + stat_in[layer, d]
        mean = jnp.broadcast_to(total[0:1], (128, tb2)).T[:, 0:1] / (kw * 2 * NX)
        gains = gain_ref[:, pl.ds(al(me_plane * kw, 128), kw)].astype(F32)
        gain = jnp.where(layer == 0, gains[0:1], gains[1:2])
        normed = (r * lax.rsqrt(mean + NORM_EPS) * gain).astype(BF16)
        own_cols = pl.ds(al((2 + c) * kw, kw), kw)
        for t in range(2):
            h_buf[yh, t, yl, :, own_cols] = normed[t * blk:(t + 1) * blk]
        mine = h_buf.at[yh, :, yl, :, own_cols]
        far = h_buf.at[yh, :, yl, :, pl.ds(al(c * kw, kw), kw)]
        send(mine, far, h_s.at[layer], h_r.at[layer], dev(tb=right, ta=0))
        send(mine, far, h_s.at[layer], h_r.at[layer], dev(tb=left, ta=1))
        for d in range(1, NY):
            send(mine, mine, y0_s.at[layer], y0_r.at[layer], dev(mp=(y + d) % NY))
        issue_all(layer, ((4, 0), (4, 1), (5, 0), (5, 1), (6, 0), (6, 1)))
        acc[...] = jnp.zeros_like(acc)
        near = h_buf.at[yh, :, yl, :, 0:2 * kw]
        wait(near, h_r.at[layer])
        for d in range(1, NY):
            send(near, near, y_s.at[layer], y_r.at[layer], dev(mp=(y + d) % NY))
        kv_spread(layer)
        wait(sized(3 * tb2), y0_r.at[layer])
        own_all = h_buf.at[:, :, :, :, own_cols]
        send(own_all, own_all, sb_s.at[layer], sb_r.at[layer], sib)
        wait(sized(6 * tb2), y_r.at[layer])
        wait(sized(tok), sb_r.at[layer])

        def piece(j, g, p):
            return m_buf.at[j, c, g, p * sub:(p + 1) * sub]

        def share(j, g, p):
            send(piece(j, g, p), piece(j, g, p), d_s.at[layer], d_r.at[layer, j, p], sib)

        def stage_m_out(j, m):
            m_buf[j, c, group] = m
            for p in range(2):
                blkref = piece(j, group, p)
                send(blkref, blkref, ring_s.at[layer], ring_r.at[layer, j, 0, p], ring)
                share(j, group, p)

        def stage_r(j, s, p):
            g = group_at(s)
            blkref = piece(j, g, p)
            wait(blkref, ring_r.at[layer, j, s - 1, p])
            if s < NX - 1:
                send(blkref, blkref, ring_s.at[layer], ring_r.at[layer, j, s, p], ring)
            share(j, g, p)

        def stage_d(j, p):
            wait(m_buf.at[j, 1 - c, :, p * sub:(p + 1) * sub], d_r.at[layer, j, p])
            lhs = jnp.concatenate([
                jnp.concatenate([m_buf[j, hf, g, p * sub:(p + 1) * sub] for g in range(NX)], axis=1) for hf in range(2)
            ], axis=0)
            out = jnp.dot(lhs, wb[j], preferred_element_type=F32)
            for hf in range(2):
                acc[hf * half + p * sub:hf * half + (p + 1) * sub, :] += out[hf * sub:(hf + 1) * sub]

        def stage_p(j):
            wait(w_ml.at[layer, j], w_r.at[layer, j])
            for n in range(2):
                zs[j, :, n * CW:(n + 1) * CW] = jnp.dot(hidden(), w_ml[layer, j, :, n * CW:(n + 1) * CW], preferred_element_type=F32)
            send(zs.at[j, far_rows], zr.at[j], p_s.at[layer, j], p_r.at[layer, j], partner)

        def stage_m(j):
            wait(zr.at[j], p_r.at[layer, j])
            z = zs[j, own_rows, :] + zr[j]
            gate = z[:, 0:CW].astype(BF16).astype(F32)
            up = z[:, CW:2 * CW].astype(BF16).astype(F32)
            stage_m_out(j, (jax.nn.silu(gate) * up).astype(BF16))

        def attn_p():
            wait(w_at.at[layer, 0:(4 * kw * gq + 2 * kw * gkv) // (gq + gkv)], wa_r.at[layer])
            wait(w_at.at[layer, 0:6 * qr, gq:gq + gkv], kvy_r.at[layer])
            za[...] = jnp.dot(hidden(), w_at[layer], preferred_element_type=F32)
            send(za.at[far_rows, 0:gq], zar, p_s.at[layer, nch], p_r.at[layer, nch], partner)
            send(za.at[pl.ds(al((1 - c) * half + y * blk, blk), blk), gq:gq + gkv], zkv, kvp_s.at[layer], kvp_r.at[layer], partner)

        yb = pl.ds(al(y * blk, blk), blk)

        def attn_m():
            wait(zkv, kvp_r.at[layer])
            kv_buf[group, yb, :] = (za[pl.ds(al(c * half + y * blk, blk), blk), gq:gq + gkv] + zkv[...]).astype(BF16)
            send(kv_buf.at[group, yb], kv_buf.at[group, yb], kv_s.at[layer], kv_r.at[layer, 0], back)
            wait(zar, p_r.at[layer, nch])
            q_buf[...] = (za[own_rows, 0:gq] + zar[...]).astype(BF16)

        def attn_r(s):
            g = group_back(s)
            blkref = kv_buf.at[g, yb]
            wait(blkref, kv_r.at[layer, s - 1])
            if s < NX - 1:
                send(blkref, blkref, kv_s.at[layer], kv_r.at[layer, s], back)
            else:
                for d in range(1, NY):
                    send(kv_buf.at[:, yb], kv_buf.at[:, yb], kvz_s.at[layer], kvz_r.at[layer], dev(mp=(y + d) % NY))

        def attn_core():
            wait(kv_buf.at[0:NX - 1], kvz_r.at[layer])
            outs = []
            for b in range(4):
                rows = slice(b * blk, (b + 1) * blk)
                q = rope(q_buf[rows, :], rows)
                k = rope(jnp.concatenate([kv_buf[0, rows, :], kv_buf[1, rows, :]], axis=1), rows)
                v = jnp.concatenate([kv_buf[2, rows, :], kv_buf[3, rows, :]], axis=1)
                scores = lax.dot_general(q, k, (((1,), (1,)), ((), ())), preferred_element_type=F32) * (gq ** -0.5)
                scores = jnp.where(packs[b, :, 0:blk].astype(F32) > 0.5, scores, -1e30)
                ex = jnp.exp(scores - jnp.max(scores, axis=1, keepdims=True))
                prob = (ex / jnp.sum(ex, axis=1, keepdims=True)).astype(BF16)
                outs.append(jnp.dot(prob, v, preferred_element_type=F32).astype(BF16))
            stage_m_out(nch, jnp.concatenate(outs, axis=0))

        last = nch - 1
        attn_p()
        for j in range(nch):
            stage_p(j)
        pl.when(layer == 0)(tables)
        attn_m()
        stage_m(0)
        attn_r(1)
        stage_m(1)
        attn_r(2)
        stage_m(2)
        attn_r(3)
        stage_m(3)
        attn_core()
        for j in range(4, nch):
            stage_m(j)
        wait(sized(tok), sb_s.at[layer])
        wait(wb, wb_r.at[layer])
        order = (0, 1, 2, 3, nch) + tuple(range(4, nch))
        up, dn, op = (y + 1) % NY, (y + NY - 1) % NY, (y + 2) % NY
        hb = blk // 2

        def part(block, p, second, rows):
            return pl.ds(al((block // 2) * half + p * sub + (block % 2) * blk + second * hb, hb), rows)

        def to_y(rows, dst, p, to):
            send(acc.at[rows], dst, rs_s.at[layer, p], rs_r.at[layer, p], dev(mp=to))

        def sum_relay(p):
            send(acc.at[part(op, p, 0, hb)], rl_in.at[p, 0], rl_s.at[layer, p, 0], rl_r.at[layer, p, 0], dev(mp=up))
            send(acc.at[part(op, p, 1, hb)], rl_in.at[p, 1], rl_s.at[layer, p, 1], rl_r.at[layer, p, 1], dev(mp=dn))

        def sum_direct(p):
            for i in range(2):
                wait(rl_in.at[p, i], rl_s.at[layer, p, i])
            to_y(part(up, p, 1, hb), rs_in.at[p, 0, hb:blk], p, up)
            to_y(part(dn, p, 0, hb), rs_in.at[p, 1, 0:hb], p, dn)

        def sum_pass(p):
            wait(rl_in.at[p, 0], rl_r.at[layer, p, 0])
            acc[part(up, p, 0, hb), :] += rl_in[p, 0]
            to_y(part(up, p, 0, hb), rs_in.at[p, 0, 0:hb], p, up)
            wait(rl_in.at[p, 1], rl_r.at[layer, p, 1])
            acc[part(dn, p, 1, hb), :] += rl_in[p, 1]
            to_y(part(dn, p, 1, hb), rs_in.at[p, 1, hb:blk], p, dn)

        def sum_end(p):
            wait(rs_in.at[p], rs_r.at[layer, p])
            rows = slice(p * blk, (p + 1) * blk)
            res[rows, :] = res[rows, :] + (acc[part(y, p, 0, blk), :] + rs_in[p, 0] + rs_in[p, 1])

            @pl.when(layer == layers - 1)
            def _():
                swap_send(p, res.at[rows], f_in.at[:, pl.ds(al(c * kw, kw), kw)], f_s, f_r)

        for s, p in ((1, 0), (2, 0), (1, 1)):
            for j in order:
                stage_r(j, s, p)
        for i, j in enumerate(order):
            stage_r(j, 3, 0)
            if i > 0:
                stage_d(order[i - 1], 0)
        stage_d(order[-1], 0)
        sum_relay(0)
        for j in order[:2]:
            stage_r(j, 2, 1)
        sum_direct(0)
        for j in order[2:4]:
            stage_r(j, 2, 1)
        sum_pass(0)
        for j in order[4:]:
            stage_r(j, 2, 1)

        @pl.when(layer < layers - 1)
        def _():
            issue_all(layer + 1, ((0, 0), (0, 1), (1, 0), (1, 1), (2, 0), (2, 1)))

        stage_r(order[0], 3, 1)
        sum_end(0)
        for i, j in enumerate(order):
            if i > 0:
                stage_r(j, 3, 1)
                stage_d(order[i - 1], 1)
        stage_d(order[-1], 1)
        sum_relay(1)
        sum_direct(1)
        sum_pass(1)
        sum_end(1)

        wait(stat_in.at[layer], st_s.at[layer])
        wait(sized(2 * tb2), h_s.at[layer])
        wait(sized(3 * tb2), y0_s.at[layer])
        wait(sized(6 * tb2), y_s.at[layer])
        for j in range(nch):
            wait(zr.at[j], p_s.at[layer, j])
        wait(zar, p_s.at[layer, nch])
        wait(kv_buf.at[0, 0:3 * blk], kv_s.at[layer])
        wait(kv_buf.at[0:NX - 1], kvz_s.at[layer])
        wait(zkv, kvp_s.at[layer])
        wait(w_at.at[layer, 0:2 * qr, gq:gq + gkv], kvx_s.at[layer])
        wait(w_at.at[layer, 0:6 * qr, gq:gq + gkv], kvy_s.at[layer])
        wait(m_buf.at[:, 0, 0:NX - 1], ring_s.at[layer])
        wait(m_buf.at[:, 0], d_s.at[layer])
        for p in range(2):
            wait(acc.at[0:2 * blk], rs_s.at[layer, p])
        wait(w_at.at[layer, 0:(3 * kw * gq + kw * gkv) // (gq + gkv)], wa_s.at[layer])
        wait(w_ml.at[layer, :, 0:3 * kw], w_s.at[layer])
        return carry

    lax.fori_loop(0, layers, layer_body, 0)

    swap_wait(res.at[0:blk], f_s, f_r)
    out_ref[...] = f_in[...]

    @pl.when(jnp.logical_not(pack_own))
    def _():
        wait(pack_ref, ps_s.at[0])

    for d in range(1, NX):
        wait(pack_ref, ps_s.at[d])


def solution(mesh):
    def device_body(x_loc, seg_ids, pos_ids, w_q, w_k, w_v, w_gate, w_up, w_out, w_down, gain):
        blk, width_loc = x_loc.shape
        layers, kw, _ = w_q.shape
        head_dim = w_k.shape[-1]
        gq = w_q.shape[-1] // NX
        gff = w_gate.shape[-1] // NX
        gkv = 2 * head_dim // NX
        nch = gff // CW
        tok, half, tb2 = 8 * blk, 4 * blk, 2 * blk
        kg = 4 * kw
        half_dim = head_dim // 2
        hbm = pl.BlockSpec(memory_space=pl.ANY)
        vmem = pl.BlockSpec(memory_space=pltpu.VMEM)
        dma = pltpu.SemaphoreType.DMA
        return pl.pallas_call(
            functools.partial(kernel, (layers, blk, kw, gq, gkv, gff)),
            out_shape=jax.ShapeDtypeStruct((blk, width_loc), F32),
            in_specs=[vmem] * 4 + [hbm] * 7,
            out_specs=vmem,
            scratch_shapes=[
                pltpu.VMEM((layers, kg, gq + gkv), BF16),
                pltpu.VMEM((layers, nch, kg, 2 * CW), BF16),
                pltpu.VMEM((nch + 1, NX * CW, kw), BF16),
                pltpu.VMEM((nch, tok, 2 * CW), F32),
                pltpu.VMEM((nch, half, 2 * CW), F32),
                pltpu.VMEM((tok, gq + gkv), F32),
                pltpu.VMEM((half, gq), F32),
                pltpu.VMEM((blk, gkv), F32),
                pltpu.VMEM((nch + 1, 2, NX, half, CW), BF16),
                pltpu.VMEM((2, 2, 2, blk, kg), BF16),
                pltpu.VMEM((tok, kw), F32),
                pltpu.VMEM((tb2, kw), F32),
                pltpu.VMEM((NX, half, gkv), BF16),
                pltpu.VMEM((half, gq), BF16),
                pltpu.VMEM((half, half_dim), F32),
                pltpu.VMEM((half, half_dim), F32),
                pltpu.VMEM((4, blk, 256), BF16),
                pltpu.VMEM((8, tb2), F32),
                pltpu.VMEM((layers, 2 * NX - 1, 8, tb2), F32),
                pltpu.VMEM((2, 2, blk, kw), F32),
                pltpu.VMEM((2, 2, blk // 2, kw), F32),
                pltpu.VMEM((tb2, kw), BF16),
                pltpu.VMEM((blk, width_loc), F32),
                pltpu.VMEM((blk, 256), BF16),
                pltpu.VMEM((128, 128), jnp.int32),
                dma((2,)), dma((2,)), dma((NX,)), dma(()),
                dma((layers,)), dma((layers,)), dma((layers, nch)), dma((layers,)), dma((layers,)),
                dma((layers, nch + 1)), dma((layers, nch + 1)),
                dma((layers,)), dma((layers, nch + 1, NX - 1, 2)), dma((layers,)), dma((layers, nch + 1, 2)),
                dma((layers,)), dma((layers, NX - 1)), dma((layers,)), dma((layers,)),
                dma((layers,)), dma((layers,)), dma((layers,)), dma((layers,)), dma((layers,)), dma((layers,)),
                dma((layers,)), dma((layers,)), dma((layers, 2)), dma((layers, 2)), dma((layers, 2, 2)), dma((layers, 2, 2)),
                dma((2,)), dma((2,)),
            ] + [dma((layers,))] * 8,
            compiler_params=pltpu.CompilerParams(collective_id=0, has_side_effects=True, vmem_limit_bytes=60 * 1024 * 1024),
        )(x_loc, seg_ids[None], pos_ids[None], gain, w_q, w_k, w_v, w_gate, w_up, w_out, w_down)

    col_spec = P(None, PLANE_AXES, "mp")
    kv_spec = P(None, PLANE_AXES, None)
    row_spec = P(None, "mp", PLANE_AXES)
    return jax.shard_map(
        device_body,
        mesh=mesh,
        in_specs=(P(TOKEN_AXES, "mp"), P(TOKEN_AXES), P(TOKEN_AXES), col_spec, kv_spec, kv_spec, col_spec, col_spec, row_spec, row_spec, P(None, None)),
        out_specs=P(TOKEN_AXES, "mp"),
        check_vma=False,
    )
```

```python
import functools
import math

import jax
import jax.numpy as jnp
from jax import lax
from jax.experimental import pallas as pl
from jax.experimental.pallas import tpu as pltpu
from jax.sharding import PartitionSpec as P

ROPE_BASE = 10000.0
NORM_EPS = 1e-6
TOKEN_AXES = ("rep", "tb", "ta")
PLANE_AXES = ("tb", "ta")
MESH = pl.DeviceIdType.MESH
BF16, F32 = jnp.bfloat16, jnp.float32
NX, NY = 4, 4
CW = 256


def al(index, unit):
    return pl.multiple_of(index, unit)


def kernel(dims, x_ref, seg_ref, pos_ref, gain_ref, wq, wk, wv, wg, wu, wo, wd, out_ref,
           w_at, w_ml, wb, zs, zr, za, zar, zkv, m_buf, h_buf, acc, res, kv_buf, q_buf, cos_t, sin_t, packs,
           stat_own, stat_in, rs_in, rl_in, x_in, pack_ref, ids_t,
           xs_s, xs_r, ps_s, ps_r, w_s, wa_s, w_r, wa_r, wb_r, p_s, p_r, ring_s, ring_r, d_s, d_r,
           kv_s, kv_r, h_s, h_r, y_s, y_r, y0_s, y0_r, sb_s, sb_r, st_s, st_r,
           rs_s, rs_r, rl_s, rl_r, f_s, f_r, kvx_s, kvx_r, kvy_s, kvy_r, kvp_s, kvp_r, kvz_s, kvz_r):
    layers, blk, kw, gq, gkv, gff = dims
    nch = gff // CW
    tok = 8 * blk
    half = tok // 2
    tb2 = 2 * blk
    x, c, y = lax.axis_index("tb"), lax.axis_index("ta"), lax.axis_index("mp")
    right, left = (x + 1) % NX, (x + NX - 1) % NX
    nxt = right * (1 - c) + left * c
    prv = left * (1 - c) + right * c
    group = (x + NX - c) % NX

    def dev(tb=None, ta=None, mp=None):
        return {"tb": x if tb is None else tb, "ta": c if ta is None else ta, "mp": y if mp is None else mp}

    sib = dev(ta=1 - c)
    ring = dev(tb=nxt)
    partner = dev(tb=nxt, ta=1 - c)

    def send(src, dst, ssem, rsem, to):
        pltpu.make_async_remote_copy(src_ref=src, dst_ref=dst, send_sem=ssem, recv_sem=rsem, device_id=to, device_id_type=MESH).start()

    def local(src, dst, sem):
        pltpu.make_async_copy(src, dst, sem).start()

    def wait(ref, sem):
        pltpu.make_async_copy(ref, ref, sem).wait()

    me_plane = 2 * x + c
    barrier = pltpu.get_barrier_semaphore()
    for d in range(1, 2 * NX):
        q = (me_plane + d) % (2 * NX)
        pl.semaphore_signal(barrier, inc=1, device_id=dev(tb=q // 2, ta=q % 2), device_id_type=MESH)
    for d in range(1, NY):
        pl.semaphore_signal(barrier, inc=1, device_id=dev(mp=(y + d) % NY), device_id_type=MESH)

    peers = 2 * NX - 1 + NY - 1

    @pl.when(x != y)
    def _():
        for t in range(2):
            pl.semaphore_signal(barrier, inc=1, device_id=dev(tb=y, ta=t, mp=x), device_id_type=MESH)
        pl.semaphore_wait(barrier, peers + 2)

    @pl.when(x == y)
    def _():
        pl.semaphore_wait(barrier, peers)

    def swap_send(t, src, dst, ssem, rsem):
        own = jnp.logical_and(x == y, c == t)

        @pl.when(own)
        def _():
            local(src, dst, rsem.at[c])

        @pl.when(jnp.logical_not(own))
        def _():
            send(src, dst, ssem.at[t], rsem.at[c], dev(tb=y, ta=t, mp=x))

    def swap_start(src_of, dst, ssem, rsem):
        for t in range(2):
            swap_send(t, src_of(t), dst, ssem, rsem)

    def swap_wait(part, ssem, rsem):
        for t in range(2):
            wait(part, rsem.at[t])

            @pl.when(jnp.logical_not(jnp.logical_and(x == y, c == t)))
            def _():
                wait(part, ssem.at[t])

    swap_start(lambda t: x_ref.at[:, t * kw:(t + 1) * kw], x_in.at[pl.ds(al(c * blk, blk), blk)], xs_s, xs_r)

    qr = kw // NY

    def kv_quarter(slot):
        return pl.ds(al(slot * kw + y * qr, qr), qr)

    def kv_spread(layer):
        wait(w_at.at[layer, 0:2 * qr, gq:gq + gkv], kvx_r.at[layer])
        for d in range(1, NY):
            for slot in range(2):
                piece = w_at.at[layer, kv_quarter(slot), gq:gq + gkv]
                send(piece, piece, kvy_s, kvy_r, dev(mp=(y + d) % NY))

    def issue_w(layer, idx, part):
        if part == 0:
            targets = (((prv + NX + c - 1) % NX, c, dev(tb=prv, ta=1 - c)), ((x + 3 + c) % NX, 2 + c, sib), (group, 2 + c, None))
        else:
            targets = (((nxt + NX - c) % NX, c, ring),)
        for grp, slot, to in targets:
            rows = pl.ds(al(slot * kw, kw), kw)

            def put(src, dst, ssem, rsem):
                if to is None:
                    local(src, dst, rsem)
                else:
                    send(src, dst, ssem, rsem, to)

            if idx == 0:
                ssem, rsem = wa_s.at[layer], wa_r.at[layer]
                put(wq.at[layer, :, pl.ds(al(grp * gq, gq), gq)], w_at.at[layer, rows, 0:gq], ssem, rsem)
                kv_cols = pl.ds(al((grp % 2) * gkv, gkv), gkv)
                if to is None or to is sib:
                    kv_src, kv_rows, kv_sems = slice(None), rows, (ssem, rsem)
                else:
                    kv_src, kv_rows, kv_sems = pl.ds(al(y * qr, qr), qr), kv_quarter(slot), (kvx_s.at[layer], kvx_r.at[layer])
                kv_dst = w_at.at[layer, kv_rows, gq:gq + gkv]

                @pl.when(grp < 2)
                def _():
                    put(wk.at[layer, kv_src, kv_cols], kv_dst, *kv_sems)

                @pl.when(grp >= 2)
                def _():
                    put(wv.at[layer, kv_src, kv_cols], kv_dst, *kv_sems)
            else:
                j = idx - 1
                cols = pl.ds(al(grp * gff + j * CW, CW), CW)
                ssem, rsem = w_s.at[layer], w_r.at[layer, j]
                put(wg.at[layer, :, cols], w_ml.at[layer, j, rows, 0:CW], ssem, rsem)
                put(wu.at[layer, :, cols], w_ml.at[layer, j, rows, CW:2 * CW], ssem, rsem)

    issue_w(0, 0, 0)
    issue_w(0, 0, 1)

    ids_t[...] = jnp.zeros_like(ids_t)
    ids_t[:, 0:blk] = jnp.broadcast_to(seg_ref[...], (128, blk))
    seg_rows, seg_cols = ids_t[0:blk, 0:blk], ids_t[...].T[0:blk, 0:blk]
    ids_t[:, 0:blk] = jnp.broadcast_to(pos_ref[...], (128, blk))
    pos_rows, pos_cols = ids_t[0:blk, 0:blk], ids_t[...].T[0:blk]
    allowed = (seg_rows == seg_cols) & (pos_rows <= pos_cols[:, 0:blk])
    pack_ref[...] = jnp.zeros_like(pack_ref)
    pack_ref[:, 0:blk] = jnp.where(allowed, 1.0, 0.0).astype(BF16)
    pack_ref[:, 128:256] = pos_cols.astype(F32).astype(BF16)

    pack_slot = c * 2 + x % 2
    pack_core = x // 2
    pack_own = c == pack_core

    @pl.when(pack_own)
    def _():
        local(pack_ref, packs.at[pack_slot], ps_r)

    @pl.when(jnp.logical_not(pack_own))
    def _():
        send(pack_ref, packs.at[pack_slot], ps_s.at[0], ps_r, dev(ta=pack_core))

    for d in range(1, NX):
        send(pack_ref, packs.at[pack_slot], ps_s.at[d], ps_r, dev(tb=(x + d) % NX, ta=pack_core))

    for idx in (1, 2):
        issue_w(0, idx, 0)
        issue_w(0, idx, 1)
    swap_wait(x_in.at[0:blk], xs_s, xs_r)
    res[...] = x_in[...].astype(F32)

    def tables():
        wait(packs, ps_r)
        lane = lax.broadcasted_iota(jnp.int32, (8, gq // 2), 1).astype(F32)
        freq = jnp.exp(lane * (-2.0 * math.log(ROPE_BASE) / gq))[0:1]
        for b in range(4):
            ang = packs[b, :, 128:256].astype(F32) * freq
            cos_t[b * blk:(b + 1) * blk, :] = jnp.cos(ang)
            sin_t[b * blk:(b + 1) * blk, :] = jnp.sin(ang)

    def rope(v, rows):
        lo, hi = v[:, 0:128].astype(F32), v[:, 128:256].astype(F32)
        cs, sn = cos_t[rows, :], sin_t[rows, :]
        return jnp.concatenate([lo * cs - hi * sn, hi * cs + lo * sn], axis=1).astype(BF16)

    own_rows = pl.ds(al(c * half, half), half)
    far_rows = pl.ds(al((1 - c) * half, half), half)
    yh, yl = y // 2, y % 2
    sub = half // 2

    def sized(rows):
        return w_at.at[0, 0:rows]

    def hidden():
        return h_buf[...].reshape(tok, 4 * kw)

    def group_at(s):
        return ((x + NX - s) * (1 - c) + (x + s - 1) * c) % NX

    def group_back(s):
        return ((x + s) * (1 - c) + (x + 2 * NX - s - 1) * c) % NX

    back = dev(tb=prv)

    def issue_all(layer, units):
        for idx, part in units:
            issue_w(layer, idx, part)

    def layer_body(layer, carry):
        for g in range(NX):
            for j in range(nch):
                local(wd.at[layer, g * gff + j * CW:g * gff + (j + 1) * CW], wb.at[j, g * CW:(g + 1) * CW], wb_r)
        local(wo.at[layer], wb.at[nch], wb_r)

        r = res[...]
        ssum = jnp.sum(r * r, axis=1, keepdims=True)
        stat = jnp.broadcast_to(ssum, (tb2, 128)).T[0:8]
        stat_own[...] = stat
        for d in range(1, 2 * NX):
            q = (me_plane + d) % (2 * NX)
            send(stat_own, stat_in.at[layer, d - 1], st_s, st_r, dev(tb=q // 2, ta=q % 2))
        issue_all(layer, ((3, 0), (3, 1)))
        wait(stat_in.at[layer], st_r)
        total = stat
        for d in range(2 * NX - 1):
            total = total + stat_in[layer, d]
        mean = jnp.broadcast_to(total[0:1], (128, tb2)).T[:, 0:1] / (kw * 2 * NX)
        gains = gain_ref[:, pl.ds(al(me_plane * kw, 128), kw)].astype(F32)
        gain = jnp.where(layer == 0, gains[0:1], gains[1:2])
        normed = (r * lax.rsqrt(mean + NORM_EPS) * gain).astype(BF16)
        own_cols = pl.ds(al((2 + c) * kw, kw), kw)
        for t in range(2):
            h_buf[yh, t, yl, :, own_cols] = normed[t * blk:(t + 1) * blk]
        mine = h_buf.at[yh, :, yl, :, own_cols]
        far = h_buf.at[yh, :, yl, :, pl.ds(al(c * kw, kw), kw)]
        send(mine, far, h_s, h_r, dev(tb=right, ta=0))
        send(mine, far, h_s, h_r, dev(tb=left, ta=1))
        for d in range(1, NY):
            send(mine, mine, y0_s, y0_r, dev(mp=(y + d) % NY))
        issue_all(layer, ((4, 0), (4, 1), (5, 0), (5, 1), (6, 0), (6, 1)))
        acc[...] = jnp.zeros_like(acc)
        near = h_buf.at[yh, :, yl, :, 0:2 * kw]
        wait(near, h_r)
        for d in range(1, NY):
            send(near, near, y_s, y_r, dev(mp=(y + d) % NY))
        kv_spread(layer)
        wait(sized(3 * tb2), y0_r)
        own_all = h_buf.at[:, :, :, :, own_cols]
        send(own_all, own_all, sb_s, sb_r, sib)
        wait(sized(6 * tb2), y_r)
        wait(sized(tok), sb_r)

        def piece(j, g, p):
            return m_buf.at[j, c, g, p * sub:(p + 1) * sub]

        def share(j, g, p):
            send(piece(j, g, p), piece(j, g, p), d_s, d_r.at[j, p], sib)

        def stage_m_out(j, m):
            m_buf[j, c, group] = m
            for p in range(2):
                blkref = piece(j, group, p)
                send(blkref, blkref, ring_s, ring_r.at[j, 0, p], ring)
                share(j, group, p)

        def stage_r(j, s, p):
            g = group_at(s)
            blkref = piece(j, g, p)
            wait(blkref, ring_r.at[j, s - 1, p])
            if s < NX - 1:
                send(blkref, blkref, ring_s, ring_r.at[j, s, p], ring)
            share(j, g, p)

        def stage_d(j, p):
            wait(m_buf.at[j, 1 - c, :, p * sub:(p + 1) * sub], d_r.at[j, p])
            lhs = jnp.concatenate([
                jnp.concatenate([m_buf[j, hf, g, p * sub:(p + 1) * sub] for g in range(NX)], axis=1) for hf in range(2)
            ], axis=0)
            out = jnp.dot(lhs, wb[j], preferred_element_type=F32)
            for hf in range(2):
                acc[hf * half + p * sub:hf * half + (p + 1) * sub, :] += out[hf * sub:(hf + 1) * sub]

        def stage_p(j):
            wait(w_ml.at[layer, j], w_r.at[layer, j])
            for n in range(2):
                zs[j, :, n * CW:(n + 1) * CW] = jnp.dot(hidden(), w_ml[layer, j, :, n * CW:(n + 1) * CW], preferred_element_type=F32)
            send(zs.at[j, far_rows], zr.at[j], p_s.at[j], p_r.at[j], partner)

        def stage_m(j):
            wait(zr.at[j], p_r.at[j])
            z = zs[j, own_rows, :] + zr[j]
            gate = z[:, 0:CW].astype(BF16).astype(F32)
            up = z[:, CW:2 * CW].astype(BF16).astype(F32)
            stage_m_out(j, (jax.nn.silu(gate) * up).astype(BF16))

        def attn_p():
            wait(w_at.at[layer, 0:(4 * kw * gq + 2 * kw * gkv) // (gq + gkv)], wa_r.at[layer])
            wait(w_at.at[layer, 0:6 * qr, gq:gq + gkv], kvy_r)
            za[...] = jnp.dot(hidden(), w_at[layer], preferred_element_type=F32)
            send(za.at[far_rows, 0:gq], zar, p_s.at[nch], p_r.at[nch], partner)
            send(za.at[pl.ds(al((1 - c) * half + y * blk, blk), blk), gq:gq + gkv], zkv, kvp_s, kvp_r, partner)

        yb = pl.ds(al(y * blk, blk), blk)

        def attn_m():
            wait(zkv, kvp_r)
            kv_buf[group, yb, :] = (za[pl.ds(al(c * half + y * blk, blk), blk), gq:gq + gkv] + zkv[...]).astype(BF16)
            send(kv_buf.at[group, yb], kv_buf.at[group, yb], kv_s, kv_r.at[0], back)
            wait(zar, p_r.at[nch])
            q_buf[...] = (za[own_rows, 0:gq] + zar[...]).astype(BF16)

        def attn_r(s):
            g = group_back(s)
            blkref = kv_buf.at[g, yb]
            wait(blkref, kv_r.at[s - 1])
            if s < NX - 1:
                send(blkref, blkref, kv_s, kv_r.at[s], back)
            else:
                for d in range(1, NY):
                    send(kv_buf.at[:, yb], kv_buf.at[:, yb], kvz_s, kvz_r, dev(mp=(y + d) % NY))

        def attn_core():
            wait(kv_buf.at[0:NX - 1], kvz_r)
            outs = []
            for b in range(4):
                rows = slice(b * blk, (b + 1) * blk)
                q = rope(q_buf[rows, :], rows)
                k = rope(jnp.concatenate([kv_buf[0, rows, :], kv_buf[1, rows, :]], axis=1), rows)
                v = jnp.concatenate([kv_buf[2, rows, :], kv_buf[3, rows, :]], axis=1)
                scores = lax.dot_general(q, k, (((1,), (1,)), ((), ())), preferred_element_type=F32) * (gq ** -0.5)
                scores = jnp.where(packs[b, :, 0:blk].astype(F32) > 0.5, scores, -1e30)
                ex = jnp.exp(scores - jnp.max(scores, axis=1, keepdims=True))
                prob = (ex / jnp.sum(ex, axis=1, keepdims=True)).astype(BF16)
                outs.append(jnp.dot(prob, v, preferred_element_type=F32).astype(BF16))
            stage_m_out(nch, jnp.concatenate(outs, axis=0))

        last = nch - 1
        attn_p()
        for j in range(nch):
            stage_p(j)
        pl.when(layer == 0)(tables)
        attn_m()
        stage_m(0)
        attn_r(1)
        stage_m(1)
        attn_r(2)
        stage_m(2)
        attn_r(3)
        stage_m(3)
        attn_core()
        for j in range(4, nch):
            stage_m(j)
        wait(sized(tok), sb_s)
        wait(wb, wb_r)
        order = (0, 1, 2, 3, nch) + tuple(range(4, nch))
        up, dn, op = (y + 1) % NY, (y + NY - 1) % NY, (y + 2) % NY
        hb = blk // 2

        def part(block, p, second, rows):
            return pl.ds(al((block // 2) * half + p * sub + (block % 2) * blk + second * hb, hb), rows)

        def to_y(rows, dst, p, to):
            send(acc.at[rows], dst, rs_s.at[p], rs_r.at[p], dev(mp=to))

        def sum_relay(p):
            send(acc.at[part(op, p, 0, hb)], rl_in.at[p, 0], rl_s.at[p, 0], rl_r.at[p, 0], dev(mp=up))
            send(acc.at[part(op, p, 1, hb)], rl_in.at[p, 1], rl_s.at[p, 1], rl_r.at[p, 1], dev(mp=dn))

        def sum_direct(p):
            for i in range(2):
                wait(rl_in.at[p, i], rl_s.at[p, i])
            to_y(part(up, p, 1, hb), rs_in.at[p, 0, hb:blk], p, up)
            to_y(part(dn, p, 0, hb), rs_in.at[p, 1, 0:hb], p, dn)

        def sum_pass(p):
            wait(rl_in.at[p, 0], rl_r.at[p, 0])
            acc[part(up, p, 0, hb), :] += rl_in[p, 0]
            to_y(part(up, p, 0, hb), rs_in.at[p, 0, 0:hb], p, up)
            wait(rl_in.at[p, 1], rl_r.at[p, 1])
            acc[part(dn, p, 1, hb), :] += rl_in[p, 1]
            to_y(part(dn, p, 1, hb), rs_in.at[p, 1, hb:blk], p, dn)

        def sum_end(p):
            wait(rs_in.at[p], rs_r.at[p])
            rows = slice(p * blk, (p + 1) * blk)
            res[rows, :] = res[rows, :] + (acc[part(y, p, 0, blk), :] + rs_in[p, 0] + rs_in[p, 1])

            @pl.when(layer == layers - 1)
            def _():
                swap_send(p, res.at[rows], out_ref.at[:, pl.ds(al(c * kw, kw), kw)], f_s, f_r)

        for s, p in ((1, 0), (2, 0), (1, 1)):
            for j in order:
                stage_r(j, s, p)
        for i, j in enumerate(order):
            stage_r(j, 3, 0)
            if i > 0:
                stage_d(order[i - 1], 0)
        stage_d(order[-1], 0)
        sum_relay(0)
        for j in order:
            stage_r(j, 2, 1)

        @pl.when(layer < layers - 1)
        def _():
            issue_all(layer + 1, ((0, 0), (0, 1), (1, 0), (1, 1), (2, 0), (2, 1)))

        sum_direct(0)
        stage_r(order[0], 3, 1)
        for i, j in enumerate(order[1:]):
            stage_r(j, 3, 1)
            stage_d(order[i], 1)
            if i == 0:
                sum_pass(0)
            if i == 3:
                sum_end(0)
        stage_d(order[-1], 1)
        sum_relay(1)
        sum_direct(1)
        sum_pass(1)
        sum_end(1)

        wait(stat_in.at[layer], st_s)
        wait(sized(2 * tb2), h_s)
        wait(sized(3 * tb2), y0_s)
        wait(sized(6 * tb2), y_s)
        for j in range(nch):
            wait(zr.at[j], p_s.at[j])
        wait(zar, p_s.at[nch])
        wait(kv_buf.at[0, 0:3 * blk], kv_s)
        wait(kv_buf.at[0:NX - 1], kvz_s)
        wait(zkv, kvp_s)
        wait(w_at.at[layer, 0:2 * qr, gq:gq + gkv], kvx_s.at[layer])
        wait(w_at.at[layer, 0:6 * qr, gq:gq + gkv], kvy_s)
        wait(m_buf.at[:, 0, 0:NX - 1], ring_s)
        wait(m_buf.at[:, 0], d_s)
        for p in range(2):
            wait(acc.at[0:2 * blk], rs_s.at[p])
        wait(w_at.at[layer, 0:(3 * kw * gq + kw * gkv) // (gq + gkv)], wa_s.at[layer])
        wait(w_ml.at[layer, :, 0:3 * kw], w_s.at[layer])
        return carry

    lax.fori_loop(0, layers, layer_body, 0)

    swap_wait(res.at[0:blk], f_s, f_r)

    @pl.when(jnp.logical_not(pack_own))
    def _():
        wait(pack_ref, ps_s.at[0])

    for d in range(1, NX):
        wait(pack_ref, ps_s.at[d])


def solution(mesh):
    def device_body(x_loc, seg_ids, pos_ids, w_q, w_k, w_v, w_gate, w_up, w_out, w_down, gain):
        blk, width_loc = x_loc.shape
        layers, kw, _ = w_q.shape
        head_dim = w_k.shape[-1]
        gq = w_q.shape[-1] // NX
        gff = w_gate.shape[-1] // NX
        gkv = 2 * head_dim // NX
        nch = gff // CW
        tok, half, tb2 = 8 * blk, 4 * blk, 2 * blk
        kg = 4 * kw
        half_dim = head_dim // 2
        hbm = pl.BlockSpec(memory_space=pl.ANY)
        vmem = pl.BlockSpec(memory_space=pltpu.VMEM)
        dma = pltpu.SemaphoreType.DMA
        return pl.pallas_call(
            functools.partial(kernel, (layers, blk, kw, gq, gkv, gff)),
            out_shape=jax.ShapeDtypeStruct((blk, width_loc), F32),
            in_specs=[vmem] * 4 + [hbm] * 7,
            out_specs=hbm,
            scratch_shapes=[
                pltpu.VMEM((layers, kg, gq + gkv), BF16),
                pltpu.VMEM((layers, nch, kg, 2 * CW), BF16),
                pltpu.VMEM((nch + 1, NX * CW, kw), BF16),
                pltpu.VMEM((nch, tok, 2 * CW), F32),
                pltpu.VMEM((nch, half, 2 * CW), F32),
                pltpu.VMEM((tok, gq + gkv), F32),
                pltpu.VMEM((half, gq), F32),
                pltpu.VMEM((blk, gkv), F32),
                pltpu.VMEM((nch + 1, 2, NX, half, CW), BF16),
                pltpu.VMEM((2, 2, 2, blk, kg), BF16),
                pltpu.VMEM((tok, kw), F32),
                pltpu.VMEM((tb2, kw), F32),
                pltpu.VMEM((NX, half, gkv), BF16),
                pltpu.VMEM((half, gq), BF16),
                pltpu.VMEM((half, half_dim), F32),
                pltpu.VMEM((half, half_dim), F32),
                pltpu.VMEM((4, blk, 256), BF16),
                pltpu.VMEM((8, tb2), F32),
                pltpu.VMEM((layers, 2 * NX - 1, 8, tb2), F32),
                pltpu.VMEM((2, 2, blk, kw), F32),
                pltpu.VMEM((2, 2, blk // 2, kw), F32),
                pltpu.VMEM((tb2, kw), BF16),
                pltpu.VMEM((blk, 256), BF16),
                pltpu.VMEM((128, 128), jnp.int32),
                dma((2,)), dma((2,)), dma((NX,)), dma(()),
                dma((layers,)), dma((layers,)), dma((layers, nch)), dma((layers,)), dma(()),
                dma((nch + 1,)), dma((nch + 1,)),
                dma(()), dma((nch + 1, NX - 1, 2)), dma(()), dma((nch + 1, 2)),
                dma(()), dma((NX - 1,)),
            ] + [dma(())] * 10 + [
                dma((2,)), dma((2,)), dma((2, 2)), dma((2, 2)), dma((2,)), dma((2,)), dma((layers,)), dma((layers,)),
            ] + [dma(())] * 6,
            compiler_params=pltpu.CompilerParams(collective_id=0, has_side_effects=True, vmem_limit_bytes=60 * 1024 * 1024),
        )(x_loc, seg_ids[None], pos_ids[None], gain, w_q, w_k, w_v, w_gate, w_up, w_out, w_down)

    col_spec = P(None, PLANE_AXES, "mp")
    kv_spec = P(None, PLANE_AXES, None)
    row_spec = P(None, "mp", PLANE_AXES)
    return jax.shard_map(
        device_body,
        mesh=mesh,
        in_specs=(P(TOKEN_AXES, "mp"), P(TOKEN_AXES), P(TOKEN_AXES), col_spec, kv_spec, kv_spec, col_spec, col_spec, row_spec, row_spec, P(None, None)),
        out_specs=P(TOKEN_AXES, "mp"),
        check_vma=False,
    )
```

```python
import functools
import math

import jax
import jax.numpy as jnp
from jax import lax
from jax.experimental import pallas as pl
from jax.experimental.pallas import tpu as pltpu
from jax.sharding import PartitionSpec as P

ROPE_BASE = 10000.0
NORM_EPS = 1e-6
TOKEN_AXES = ("rep", "tb", "ta")
PLANE_AXES = ("tb", "ta")
MESH = pl.DeviceIdType.MESH
BF16, F32 = jnp.bfloat16, jnp.float32
NX, NY = 4, 4
CW = 256


def al(index, unit):
    return pl.multiple_of(index, unit)


def kernel(dims, x_ref, seg_hbm, pos_hbm, gain_hbm, wq, wk, wv, wg, wu, wo, wd, out_ref,
           w_at, w_ml, wb, zs, zr, za, zar, zkv, m_buf, h_buf, acc, res, kv_buf, q_buf, cos_t, sin_t, packs,
           stat_own, stat_in, rs_in, rl_in, x_in, pack_ref, ids_t, seg_ref, pos_ref, gain_ref,
           xs_s, xs_r, ps_s, ps_r, w_s, wa_s, w_r, wa_r, wb_r, p_s, p_r, ring_s, ring_r, d_s, d_r,
           kv_s, kv_r, h_s, h_r, y_s, y_r, y0_s, y0_r, sb_s, sb_r, st_s, st_r,
           rs_s, rs_r, rl_s, rl_r, f_s, f_r, kvx_s, kvx_r, kvy_s, kvy_r, kvp_s, kvp_r, kvz_s, kvz_r, in_r):
    layers, blk, kw, gq, gkv, gff = dims
    nch = gff // CW
    tok = 8 * blk
    half = tok // 2
    tb2 = 2 * blk
    x, c, y = lax.axis_index("tb"), lax.axis_index("ta"), lax.axis_index("mp")
    right, left = (x + 1) % NX, (x + NX - 1) % NX
    nxt = right * (1 - c) + left * c
    prv = left * (1 - c) + right * c
    group = (x + NX - c) % NX

    def dev(tb=None, ta=None, mp=None):
        return {"tb": x if tb is None else tb, "ta": c if ta is None else ta, "mp": y if mp is None else mp}

    sib = dev(ta=1 - c)
    ring = dev(tb=nxt)
    partner = dev(tb=nxt, ta=1 - c)

    def send(src, dst, ssem, rsem, to):
        pltpu.make_async_remote_copy(src_ref=src, dst_ref=dst, send_sem=ssem, recv_sem=rsem, device_id=to, device_id_type=MESH).start()

    def local(src, dst, sem):
        pltpu.make_async_copy(src, dst, sem).start()

    def wait(ref, sem):
        pltpu.make_async_copy(ref, ref, sem).wait()

    small = ((seg_hbm, seg_ref), (pos_hbm, pos_ref), (gain_hbm, gain_ref))
    for i, (src, dst) in enumerate(small):
        local(src, dst, in_r.at[i])
    me_plane = 2 * x + c
    barrier = pltpu.get_barrier_semaphore()
    for d in range(1, 2 * NX):
        q = (me_plane + d) % (2 * NX)
        pl.semaphore_signal(barrier, inc=1, device_id=dev(tb=q // 2, ta=q % 2), device_id_type=MESH)
    for d in range(1, NY):
        pl.semaphore_signal(barrier, inc=1, device_id=dev(mp=(y + d) % NY), device_id_type=MESH)

    peers = 2 * NX - 1 + NY - 1

    @pl.when(x != y)
    def _():
        for t in range(2):
            pl.semaphore_signal(barrier, inc=1, device_id=dev(tb=y, ta=t, mp=x), device_id_type=MESH)
        pl.semaphore_wait(barrier, peers + 2)

    @pl.when(x == y)
    def _():
        pl.semaphore_wait(barrier, peers)

    def swap_send(t, src, dst, ssem, rsem):
        own = jnp.logical_and(x == y, c == t)

        @pl.when(own)
        def _():
            local(src, dst, rsem.at[c])

        @pl.when(jnp.logical_not(own))
        def _():
            send(src, dst, ssem.at[t], rsem.at[c], dev(tb=y, ta=t, mp=x))

    def swap_start(src_of, dst, ssem, rsem):
        for t in range(2):
            swap_send(t, src_of(t), dst, ssem, rsem)

    def swap_wait(part, ssem, rsem):
        for t in range(2):
            wait(part, rsem.at[t])

            @pl.when(jnp.logical_not(jnp.logical_and(x == y, c == t)))
            def _():
                wait(part, ssem.at[t])

    swap_start(lambda t: x_ref.at[:, t * kw:(t + 1) * kw], x_in.at[pl.ds(al(c * blk, blk), blk)], xs_s, xs_r)

    qr = kw // NY

    def kv_quarter(slot):
        return pl.ds(al(slot * kw + y * qr, qr), qr)

    def kv_spread(layer):
        wait(w_at.at[layer, 0:2 * qr, gq:gq + gkv], kvx_r.at[layer])
        for d in range(1, NY):
            for slot in range(2):
                piece = w_at.at[layer, kv_quarter(slot), gq:gq + gkv]
                send(piece, piece, kvy_s, kvy_r, dev(mp=(y + d) % NY))

    def issue_w(layer, idx, part):
        if part == 0:
            targets = (((prv + NX + c - 1) % NX, c, dev(tb=prv, ta=1 - c)), ((x + 3 + c) % NX, 2 + c, sib), (group, 2 + c, None))
        else:
            targets = (((nxt + NX - c) % NX, c, ring),)
        for grp, slot, to in targets:
            rows = pl.ds(al(slot * kw, kw), kw)

            def put(src, dst, ssem, rsem):
                if to is None:
                    local(src, dst, rsem)
                else:
                    send(src, dst, ssem, rsem, to)

            if idx == 0:
                ssem, rsem = wa_s.at[layer], wa_r.at[layer]
                put(wq.at[layer, :, pl.ds(al(grp * gq, gq), gq)], w_at.at[layer, rows, 0:gq], ssem, rsem)
                kv_cols = pl.ds(al((grp % 2) * gkv, gkv), gkv)
                if to is None or to is sib:
                    kv_src, kv_rows, kv_sems = slice(None), rows, (ssem, rsem)
                else:
                    kv_src, kv_rows, kv_sems = pl.ds(al(y * qr, qr), qr), kv_quarter(slot), (kvx_s.at[layer], kvx_r.at[layer])
                kv_dst = w_at.at[layer, kv_rows, gq:gq + gkv]

                @pl.when(grp < 2)
                def _():
                    put(wk.at[layer, kv_src, kv_cols], kv_dst, *kv_sems)

                @pl.when(grp >= 2)
                def _():
                    put(wv.at[layer, kv_src, kv_cols], kv_dst, *kv_sems)
            else:
                j = idx - 1
                cols = pl.ds(al(grp * gff + j * CW, CW), CW)
                ssem, rsem = w_s.at[layer], w_r.at[layer, j]
                put(wg.at[layer, :, cols], w_ml.at[layer, j, rows, 0:CW], ssem, rsem)
                put(wu.at[layer, :, cols], w_ml.at[layer, j, rows, CW:2 * CW], ssem, rsem)

    issue_w(0, 0, 0)
    issue_w(0, 0, 1)

    for i, (_, dst) in enumerate(small):
        wait(dst, in_r.at[i])
    ids_t[...] = jnp.zeros_like(ids_t)
    ids_t[:, 0:blk] = jnp.broadcast_to(seg_ref[...], (128, blk))
    seg_rows, seg_cols = ids_t[0:blk, 0:blk], ids_t[...].T[0:blk, 0:blk]
    ids_t[:, 0:blk] = jnp.broadcast_to(pos_ref[...], (128, blk))
    pos_rows, pos_cols = ids_t[0:blk, 0:blk], ids_t[...].T[0:blk]
    allowed = (seg_rows == seg_cols) & (pos_rows <= pos_cols[:, 0:blk])
    pack_ref[...] = jnp.zeros_like(pack_ref)
    pack_ref[:, 0:blk] = jnp.where(allowed, 1.0, 0.0).astype(BF16)
    pack_ref[:, 128:256] = pos_cols.astype(F32).astype(BF16)

    pack_slot = c * 2 + x % 2
    pack_core = x // 2
    pack_own = c == pack_core

    @pl.when(pack_own)
    def _():
        local(pack_ref, packs.at[pack_slot], ps_r)

    @pl.when(jnp.logical_not(pack_own))
    def _():
        send(pack_ref, packs.at[pack_slot], ps_s.at[0], ps_r, dev(ta=pack_core))

    for d in range(1, NX):
        send(pack_ref, packs.at[pack_slot], ps_s.at[d], ps_r, dev(tb=(x + d) % NX, ta=pack_core))

    for idx in (1, 2):
        issue_w(0, idx, 0)
        issue_w(0, idx, 1)
    swap_wait(x_in.at[0:blk], xs_s, xs_r)
    res[...] = x_in[...].astype(F32)

    def tables():
        wait(packs, ps_r)
        lane = lax.broadcasted_iota(jnp.int32, (8, gq // 2), 1).astype(F32)
        freq = jnp.exp(lane * (-2.0 * math.log(ROPE_BASE) / gq))[0:1]
        for b in range(4):
            ang = packs[b, :, 128:256].astype(F32) * freq
            cos_t[b * blk:(b + 1) * blk, :] = jnp.cos(ang)
            sin_t[b * blk:(b + 1) * blk, :] = jnp.sin(ang)

    def rope(v, rows):
        lo, hi = v[:, 0:128].astype(F32), v[:, 128:256].astype(F32)
        cs, sn = cos_t[rows, :], sin_t[rows, :]
        return jnp.concatenate([lo * cs - hi * sn, hi * cs + lo * sn], axis=1).astype(BF16)

    own_rows = pl.ds(al(c * half, half), half)
    far_rows = pl.ds(al((1 - c) * half, half), half)
    yh, yl = y // 2, y % 2
    sub = half // 2

    def sized(rows):
        return w_at.at[0, 0:rows]

    def hidden():
        return h_buf[...].reshape(tok, 4 * kw)

    def group_at(s):
        return ((x + NX - s) * (1 - c) + (x + s - 1) * c) % NX

    def group_back(s):
        return ((x + s) * (1 - c) + (x + 2 * NX - s - 1) * c) % NX

    back = dev(tb=prv)

    def issue_all(layer, units):
        for idx, part in units:
            issue_w(layer, idx, part)

    def layer_body(layer, carry):
        for g in range(NX):
            for j in range(nch):
                local(wd.at[layer, g * gff + j * CW:g * gff + (j + 1) * CW], wb.at[j, g * CW:(g + 1) * CW], wb_r)
        local(wo.at[layer], wb.at[nch], wb_r)

        r = res[...]
        ssum = jnp.sum(r * r, axis=1, keepdims=True)
        stat = jnp.broadcast_to(ssum, (tb2, 128)).T[0:8]
        stat_own[...] = stat
        for d in range(1, 2 * NX):
            q = (me_plane + d) % (2 * NX)
            send(stat_own, stat_in.at[layer, d - 1], st_s, st_r, dev(tb=q // 2, ta=q % 2))
        issue_all(layer, ((3, 0), (3, 1)))
        wait(stat_in.at[layer], st_r)
        total = stat
        for d in range(2 * NX - 1):
            total = total + stat_in[layer, d]
        mean = jnp.broadcast_to(total[0:1], (128, tb2)).T[:, 0:1] / (kw * 2 * NX)
        gains = gain_ref[:, pl.ds(al(me_plane * kw, 128), kw)].astype(F32)
        gain = jnp.where(layer == 0, gains[0:1], gains[1:2])
        normed = (r * lax.rsqrt(mean + NORM_EPS) * gain).astype(BF16)
        own_cols = pl.ds(al((2 + c) * kw, kw), kw)
        for t in range(2):
            h_buf[yh, t, yl, :, own_cols] = normed[t * blk:(t + 1) * blk]
        mine = h_buf.at[yh, :, yl, :, own_cols]
        far = h_buf.at[yh, :, yl, :, pl.ds(al(c * kw, kw), kw)]
        send(mine, far, h_s, h_r, dev(tb=right, ta=0))
        send(mine, far, h_s, h_r, dev(tb=left, ta=1))
        for d in range(1, NY):
            send(mine, mine, y0_s, y0_r, dev(mp=(y + d) % NY))
        issue_all(layer, ((4, 0), (4, 1), (5, 0), (5, 1), (6, 0), (6, 1)))
        acc[...] = jnp.zeros_like(acc)
        near = h_buf.at[yh, :, yl, :, 0:2 * kw]
        wait(near, h_r)
        for d in range(1, NY):
            send(near, near, y_s, y_r, dev(mp=(y + d) % NY))
        kv_spread(layer)
        wait(sized(3 * tb2), y0_r)
        own_all = h_buf.at[:, :, :, :, own_cols]
        send(own_all, own_all, sb_s, sb_r, sib)
        wait(sized(6 * tb2), y_r)
        wait(sized(tok), sb_r)

        def piece(j, g, p):
            return m_buf.at[j, c, g, p * sub:(p + 1) * sub]

        def share(j, g, p):
            send(piece(j, g, p), piece(j, g, p), d_s, d_r.at[j, p], sib)

        def stage_m_out(j, m):
            m_buf[j, c, group] = m
            for p in range(2):
                blkref = piece(j, group, p)
                send(blkref, blkref, ring_s, ring_r.at[j, 0, p], ring)
                share(j, group, p)

        def stage_r(j, s, p):
            g = group_at(s)
            blkref = piece(j, g, p)
            wait(blkref, ring_r.at[j, s - 1, p])
            if s < NX - 1:
                send(blkref, blkref, ring_s, ring_r.at[j, s, p], ring)
            share(j, g, p)

        def stage_d(j, p):
            wait(m_buf.at[j, 1 - c, :, p * sub:(p + 1) * sub], d_r.at[j, p])
            lhs = jnp.concatenate([
                jnp.concatenate([m_buf[j, hf, g, p * sub:(p + 1) * sub] for g in range(NX)], axis=1) for hf in range(2)
            ], axis=0)
            out = jnp.dot(lhs, wb[j], preferred_element_type=F32)
            for hf in range(2):
                acc[hf * half + p * sub:hf * half + (p + 1) * sub, :] += out[hf * sub:(hf + 1) * sub]

        def stage_p(j):
            wait(w_ml.at[layer, j], w_r.at[layer, j])
            for n in range(2):
                zs[j, :, n * CW:(n + 1) * CW] = jnp.dot(hidden(), w_ml[layer, j, :, n * CW:(n + 1) * CW], preferred_element_type=F32)
            send(zs.at[j, far_rows], zr.at[j], p_s.at[j], p_r.at[j], partner)

        def stage_m(j):
            wait(zr.at[j], p_r.at[j])
            z = zs[j, own_rows, :] + zr[j]
            gate = z[:, 0:CW].astype(BF16).astype(F32)
            up = z[:, CW:2 * CW].astype(BF16).astype(F32)
            stage_m_out(j, (jax.nn.silu(gate) * up).astype(BF16))

        def attn_p():
            wait(w_at.at[layer, 0:(4 * kw * gq + 2 * kw * gkv) // (gq + gkv)], wa_r.at[layer])
            wait(w_at.at[layer, 0:6 * qr, gq:gq + gkv], kvy_r)
            za[...] = jnp.dot(hidden(), w_at[layer], preferred_element_type=F32)
            send(za.at[far_rows, 0:gq], zar, p_s.at[nch], p_r.at[nch], partner)
            send(za.at[pl.ds(al((1 - c) * half + y * blk, blk), blk), gq:gq + gkv], zkv, kvp_s, kvp_r, partner)

        yb = pl.ds(al(y * blk, blk), blk)

        def attn_m():
            wait(zkv, kvp_r)
            kv_buf[group, yb, :] = (za[pl.ds(al(c * half + y * blk, blk), blk), gq:gq + gkv] + zkv[...]).astype(BF16)
            send(kv_buf.at[group, yb], kv_buf.at[group, yb], kv_s, kv_r.at[0], back)
            wait(zar, p_r.at[nch])
            q_buf[...] = (za[own_rows, 0:gq] + zar[...]).astype(BF16)

        def attn_r(s):
            g = group_back(s)
            blkref = kv_buf.at[g, yb]
            wait(blkref, kv_r.at[s - 1])
            if s < NX - 1:
                send(blkref, blkref, kv_s, kv_r.at[s], back)
            else:
                for d in range(1, NY):
                    send(kv_buf.at[:, yb], kv_buf.at[:, yb], kvz_s, kvz_r, dev(mp=(y + d) % NY))

        def attn_core():
            wait(kv_buf.at[0:NX - 1], kvz_r)
            outs = []
            for b in range(4):
                rows = slice(b * blk, (b + 1) * blk)
                q = rope(q_buf[rows, :], rows)
                k = rope(jnp.concatenate([kv_buf[0, rows, :], kv_buf[1, rows, :]], axis=1), rows)
                v = jnp.concatenate([kv_buf[2, rows, :], kv_buf[3, rows, :]], axis=1)
                scores = lax.dot_general(q, k, (((1,), (1,)), ((), ())), preferred_element_type=F32) * (gq ** -0.5)
                scores = jnp.where(packs[b, :, 0:blk].astype(F32) > 0.5, scores, -1e30)
                ex = jnp.exp(scores - jnp.max(scores, axis=1, keepdims=True))
                prob = (ex / jnp.sum(ex, axis=1, keepdims=True)).astype(BF16)
                outs.append(jnp.dot(prob, v, preferred_element_type=F32).astype(BF16))
            stage_m_out(nch, jnp.concatenate(outs, axis=0))

        last = nch - 1
        attn_p()
        for j in range(nch):
            stage_p(j)
        pl.when(layer == 0)(tables)
        attn_m()
        stage_m(0)
        attn_r(1)
        stage_m(1)
        attn_r(2)
        stage_m(2)
        attn_r(3)
        stage_m(3)
        attn_core()
        for j in range(4, nch):
            stage_m(j)
        wait(sized(tok), sb_s)
        wait(wb, wb_r)
        order = (0, 1, 2, 3, nch) + tuple(range(4, nch))
        up, dn, op = (y + 1) % NY, (y + NY - 1) % NY, (y + 2) % NY
        cuts = ((0, 0, blk), (1, 0, blk // 2), (1, blk // 2, blk // 2))

        def part(block, k, second, rows):
            p, off, size = cuts[k]
            return pl.ds(al((block // 2) * half + p * sub + (block % 2) * blk + off + second * (size // 2), size // 2), rows)

        def span(k, second=None):
            p, off, size = cuts[k]
            first = p * blk + off
            if second is None:
                return slice(first, first + size)
            return slice(first + second * size // 2, first + (second + 1) * size // 2)

        def relay_span(k):
            p, off, size = cuts[k]
            return slice((p * blk + off) // 2, (p * blk + off + size) // 2)

        def to_y(rows, dst, k, to):
            send(acc.at[rows], dst, rs_s.at[k], rs_r.at[k], dev(mp=to))

        def sum_relay(k):
            hb = cuts[k][2] // 2
            send(acc.at[part(op, k, 0, hb)], rl_in.at[0, relay_span(k)], rl_s.at[k, 0], rl_r.at[k, 0], dev(mp=up))
            send(acc.at[part(op, k, 1, hb)], rl_in.at[1, relay_span(k)], rl_s.at[k, 1], rl_r.at[k, 1], dev(mp=dn))

        def sum_direct(k):
            hb = cuts[k][2] // 2
            for i in range(2):
                wait(rl_in.at[i, relay_span(k)], rl_s.at[k, i])
            to_y(part(up, k, 1, hb), rs_in.at[0, span(k, 1)], k, up)
            to_y(part(dn, k, 0, hb), rs_in.at[1, span(k, 0)], k, dn)

        def sum_pass(k):
            hb = cuts[k][2] // 2
            wait(rl_in.at[0, relay_span(k)], rl_r.at[k, 0])
            acc[part(up, k, 0, hb), :] += rl_in[0, relay_span(k)]
            to_y(part(up, k, 0, hb), rs_in.at[0, span(k, 0)], k, up)
            wait(rl_in.at[1, relay_span(k)], rl_r.at[k, 1])
            acc[part(dn, k, 1, hb), :] += rl_in[1, relay_span(k)]
            to_y(part(dn, k, 1, hb), rs_in.at[1, span(k, 1)], k, dn)

        def sum_end(k):
            p, off, size = cuts[k]
            wait(rs_in.at[0:2, span(k)], rs_r.at[k])
            res[span(k), :] = res[span(k), :] + (acc[part(y, k, 0, size), :] + rs_in[0, span(k)] + rs_in[1, span(k)])

            @pl.when(layer == layers - 1)
            def _():
                swap_send(p, res.at[span(k)], out_ref.at[off:off + size, pl.ds(al(c * kw, kw), kw)], f_s, f_r)

        for s, p in ((1, 0), (2, 0), (1, 1)):
            for j in order:
                stage_r(j, s, p)
        for i, j in enumerate(order):
            stage_r(j, 3, 0)
            if i > 0:
                stage_d(order[i - 1], 0)
        stage_d(order[-1], 0)
        sum_relay(0)
        for j in order:
            stage_r(j, 2, 1)

        @pl.when(layer < layers - 1)
        def _():
            issue_all(layer + 1, ((0, 0), (0, 1), (1, 0), (1, 1), (2, 0), (2, 1)))

        sum_direct(0)
        stage_r(order[0], 3, 1)
        for i, j in enumerate(order[1:]):
            stage_r(j, 3, 1)
            stage_d(order[i], 1)
            if i == 0:
                sum_pass(0)
            if i == 3:
                sum_end(0)
        stage_d(order[-1], 1)
        for step in (sum_relay, sum_direct, sum_pass, sum_end):
            for k in (1, 2):
                step(k)

        wait(stat_in.at[layer], st_s)
        wait(sized(2 * tb2), h_s)
        wait(sized(3 * tb2), y0_s)
        wait(sized(6 * tb2), y_s)
        for j in range(nch):
            wait(zr.at[j], p_s.at[j])
        wait(zar, p_s.at[nch])
        wait(kv_buf.at[0, 0:3 * blk], kv_s)
        wait(kv_buf.at[0:NX - 1], kvz_s)
        wait(zkv, kvp_s)
        wait(w_at.at[layer, 0:2 * qr, gq:gq + gkv], kvx_s.at[layer])
        wait(w_at.at[layer, 0:6 * qr, gq:gq + gkv], kvy_s)
        wait(m_buf.at[:, 0, 0:NX - 1], ring_s)
        wait(m_buf.at[:, 0], d_s)
        for k in range(3):
            wait(acc.at[0:2 * cuts[k][2]], rs_s.at[k])
        wait(w_at.at[layer, 0:(3 * kw * gq + kw * gkv) // (gq + gkv)], wa_s.at[layer])
        wait(w_ml.at[layer, :, 0:3 * kw], w_s.at[layer])
        return carry

    lax.fori_loop(0, layers, layer_body, 0)

    swap_wait(res.at[0:blk], f_s, f_r)

    @pl.when(jnp.logical_not(pack_own))
    def _():
        wait(pack_ref, ps_s.at[0])

    for d in range(1, NX):
        wait(pack_ref, ps_s.at[d])


def solution(mesh):
    def device_body(x_loc, seg_ids, pos_ids, w_q, w_k, w_v, w_gate, w_up, w_out, w_down, gain):
        blk, width_loc = x_loc.shape
        layers, kw, _ = w_q.shape
        head_dim = w_k.shape[-1]
        gq = w_q.shape[-1] // NX
        gff = w_gate.shape[-1] // NX
        gkv = 2 * head_dim // NX
        nch = gff // CW
        tok, half, tb2 = 8 * blk, 4 * blk, 2 * blk
        kg = 4 * kw
        half_dim = head_dim // 2
        hbm = pl.BlockSpec(memory_space=pl.ANY)
        dma = pltpu.SemaphoreType.DMA
        return pl.pallas_call(
            functools.partial(kernel, (layers, blk, kw, gq, gkv, gff)),
            out_shape=jax.ShapeDtypeStruct((blk, width_loc), F32),
            in_specs=[hbm] * 11,
            out_specs=hbm,
            scratch_shapes=[
                pltpu.VMEM((layers, kg, gq + gkv), BF16),
                pltpu.VMEM((layers, nch, kg, 2 * CW), BF16),
                pltpu.VMEM((nch + 1, NX * CW, kw), BF16),
                pltpu.VMEM((nch, tok, 2 * CW), F32),
                pltpu.VMEM((nch, half, 2 * CW), F32),
                pltpu.VMEM((tok, gq + gkv), F32),
                pltpu.VMEM((half, gq), F32),
                pltpu.VMEM((blk, gkv), F32),
                pltpu.VMEM((nch + 1, 2, NX, half, CW), BF16),
                pltpu.VMEM((2, 2, 2, blk, kg), BF16),
                pltpu.VMEM((tok, kw), F32),
                pltpu.VMEM((tb2, kw), F32),
                pltpu.VMEM((NX, half, gkv), BF16),
                pltpu.VMEM((half, gq), BF16),
                pltpu.VMEM((half, half_dim), F32),
                pltpu.VMEM((half, half_dim), F32),
                pltpu.VMEM((4, blk, 256), BF16),
                pltpu.VMEM((8, tb2), F32),
                pltpu.VMEM((layers, 2 * NX - 1, 8, tb2), F32),
                pltpu.VMEM((2, tb2, kw), F32),
                pltpu.VMEM((2, blk, kw), F32),
                pltpu.VMEM((tb2, kw), BF16),
                pltpu.VMEM((blk, 256), BF16),
                pltpu.VMEM((128, 128), jnp.int32),
                pltpu.VMEM((1, blk), jnp.int32),
                pltpu.VMEM((1, blk), jnp.int32),
                pltpu.VMEM(gain.shape, BF16),
                dma((2,)), dma((2,)), dma((NX,)), dma(()),
                dma((layers,)), dma((layers,)), dma((layers, nch)), dma((layers,)), dma(()),
                dma((nch + 1,)), dma((nch + 1,)),
                dma(()), dma((nch + 1, NX - 1, 2)), dma(()), dma((nch + 1, 2)),
                dma(()), dma((NX - 1,)),
            ] + [dma(())] * 10 + [
                dma((3,)), dma((3,)), dma((3, 2)), dma((3, 2)), dma((2,)), dma((2,)), dma((layers,)), dma((layers,)),
            ] + [dma(())] * 6 + [dma((3,))],
            compiler_params=pltpu.CompilerParams(collective_id=0, has_side_effects=True, vmem_limit_bytes=60 * 1024 * 1024),
        )(x_loc, seg_ids[None], pos_ids[None], gain, w_q, w_k, w_v, w_gate, w_up, w_out, w_down)

    col_spec = P(None, PLANE_AXES, "mp")
    kv_spec = P(None, PLANE_AXES, None)
    row_spec = P(None, "mp", PLANE_AXES)
    return jax.shard_map(
        device_body,
        mesh=mesh,
        in_specs=(P(TOKEN_AXES, "mp"), P(TOKEN_AXES), P(TOKEN_AXES), col_spec, kv_spec, kv_spec, col_spec, col_spec, row_spec, row_spec, P(None, None)),
        out_specs=P(TOKEN_AXES, "mp"),
        check_vma=False,
    )
```

```python
import functools
import math

import jax
import jax.numpy as jnp
from jax import lax
from jax.experimental import pallas as pl
from jax.experimental.pallas import tpu as pltpu
from jax.sharding import PartitionSpec as P

ROPE_BASE = 10000.0
NORM_EPS = 1e-6
TOKEN_AXES = ("rep", "tb", "ta")
PLANE_AXES = ("tb", "ta")
MESH = pl.DeviceIdType.MESH
BF16, F32 = jnp.bfloat16, jnp.float32
NX, NY = 4, 4
CW = 256


def al(index, unit):
    return pl.multiple_of(index, unit)


def kernel(dims, x_ref, seg_hbm, pos_hbm, gain_hbm, wq, wk, wv, wg, wu, wo, wd, out_ref,
           w_at, w_ml, wb, zs, zr, za, zar, zkv, m_buf, h_buf, acc, res, kv_buf, q_buf, cos_t, sin_t, packs,
           stat_own, stat_in, rs_in, rl_in, x_in, pack_ref, ids_t, seg_ref, pos_ref, gain_ref,
           xs_s, xs_r, ps_s, ps_r, w_s, wa_s, w_r, wa_r, wb_r, p_s, p_r, ring_s, ring_r, d_s, d_r,
           kv_s, kv_r, h_s, h_r, y_s, y_r, y0_s, y0_r, sb_s, sb_r, st_s, st_r,
           rs_s, rs_r, rl_s, rl_r, f_s, f_r, kvx_s, kvx_r, kvy_s, kvy_r, kvp_s, kvp_r, kvz_s, kvz_r, in_r):
    layers, blk, kw, gq, gkv, gff = dims
    nch = gff // CW
    tok = 8 * blk
    half = tok // 2
    tb2 = 2 * blk
    x, c, y = lax.axis_index("tb"), lax.axis_index("ta"), lax.axis_index("mp")
    right, left = (x + 1) % NX, (x + NX - 1) % NX
    nxt = right * (1 - c) + left * c
    prv = left * (1 - c) + right * c
    group = (x + NX - c) % NX

    def dev(tb=None, ta=None, mp=None):
        return {"tb": x if tb is None else tb, "ta": c if ta is None else ta, "mp": y if mp is None else mp}

    sib = dev(ta=1 - c)
    ring = dev(tb=nxt)
    partner = dev(tb=nxt, ta=1 - c)

    def send(src, dst, ssem, rsem, to):
        pltpu.make_async_remote_copy(src_ref=src, dst_ref=dst, send_sem=ssem, recv_sem=rsem, device_id=to, device_id_type=MESH).start()

    def local(src, dst, sem):
        pltpu.make_async_copy(src, dst, sem).start()

    def wait(ref, sem):
        pltpu.make_async_copy(ref, ref, sem).wait()

    small = ((seg_hbm, seg_ref), (pos_hbm, pos_ref), (gain_hbm, gain_ref))
    for i, (src, dst) in enumerate(small):
        local(src, dst, in_r.at[i])
    me_plane = 2 * x + c
    barrier = pltpu.get_barrier_semaphore()
    for d in range(1, 2 * NX):
        q = (me_plane + d) % (2 * NX)
        pl.semaphore_signal(barrier, inc=1, device_id=dev(tb=q // 2, ta=q % 2), device_id_type=MESH)
    for d in range(1, NY):
        pl.semaphore_signal(barrier, inc=1, device_id=dev(mp=(y + d) % NY), device_id_type=MESH)

    peers = 2 * NX - 1 + NY - 1

    @pl.when(x != y)
    def _():
        for t in range(2):
            pl.semaphore_signal(barrier, inc=1, device_id=dev(tb=y, ta=t, mp=x), device_id_type=MESH)
        pl.semaphore_wait(barrier, peers + 2)

    @pl.when(x == y)
    def _():
        pl.semaphore_wait(barrier, peers)

    def swap_send(t, src, dst, ssem, rsem):
        own = jnp.logical_and(x == y, c == t)

        @pl.when(own)
        def _():
            local(src, dst, rsem.at[c])

        @pl.when(jnp.logical_not(own))
        def _():
            send(src, dst, ssem.at[t], rsem.at[c], dev(tb=y, ta=t, mp=x))

    def swap_start(src_of, dst, ssem, rsem):
        for t in range(2):
            swap_send(t, src_of(t), dst, ssem, rsem)

    def swap_wait(part, ssem, rsem):
        for t in range(2):
            wait(part, rsem.at[t])

            @pl.when(jnp.logical_not(jnp.logical_and(x == y, c == t)))
            def _():
                wait(part, ssem.at[t])

    swap_start(lambda t: x_ref.at[:, t * kw:(t + 1) * kw], x_in.at[pl.ds(al(c * blk, blk), blk)], xs_s, xs_r)

    qr = kw // NY

    def kv_quarter(slot):
        return pl.ds(al(slot * kw + y * qr, qr), qr)

    def kv_spread(layer):
        wait(w_at.at[layer, 0:2 * qr, gq:gq + gkv], kvx_r.at[layer])
        for d in range(1, NY):
            for slot in range(2):
                piece = w_at.at[layer, kv_quarter(slot), gq:gq + gkv]
                send(piece, piece, kvy_s, kvy_r, dev(mp=(y + d) % NY))

    def issue_w(layer, idx, part):
        if part == 0:
            targets = (((prv + NX + c - 1) % NX, c, dev(tb=prv, ta=1 - c)), ((x + 3 + c) % NX, 2 + c, sib), (group, 2 + c, None))
        else:
            targets = (((nxt + NX - c) % NX, c, ring),)
        for grp, slot, to in targets:
            rows = pl.ds(al(slot * kw, kw), kw)

            def put(src, dst, ssem, rsem):
                if to is None:
                    local(src, dst, rsem)
                else:
                    send(src, dst, ssem, rsem, to)

            if idx == 0:
                ssem, rsem = wa_s.at[layer], wa_r.at[layer]
                put(wq.at[layer, :, pl.ds(al(grp * gq, gq), gq)], w_at.at[layer, rows, 0:gq], ssem, rsem)
                kv_cols = pl.ds(al((grp % 2) * gkv, gkv), gkv)
                if to is None or to is sib:
                    kv_src, kv_rows, kv_sems = slice(None), rows, (ssem, rsem)
                else:
                    kv_src, kv_rows, kv_sems = pl.ds(al(y * qr, qr), qr), kv_quarter(slot), (kvx_s.at[layer], kvx_r.at[layer])
                kv_dst = w_at.at[layer, kv_rows, gq:gq + gkv]

                @pl.when(grp < 2)
                def _():
                    put(wk.at[layer, kv_src, kv_cols], kv_dst, *kv_sems)

                @pl.when(grp >= 2)
                def _():
                    put(wv.at[layer, kv_src, kv_cols], kv_dst, *kv_sems)
            else:
                j = idx - 1
                cols = pl.ds(al(grp * gff + j * CW, CW), CW)
                ssem, rsem = w_s.at[layer], w_r.at[layer, j]
                put(wg.at[layer, :, cols], w_ml.at[layer, j, rows, 0:CW], ssem, rsem)
                put(wu.at[layer, :, cols], w_ml.at[layer, j, rows, CW:2 * CW], ssem, rsem)

    issue_w(0, 0, 0)
    issue_w(0, 0, 1)

    for i, (_, dst) in enumerate(small):
        wait(dst, in_r.at[i])
    ids_t[...] = jnp.zeros_like(ids_t)
    ids_t[:, 0:blk] = jnp.broadcast_to(seg_ref[...], (128, blk))
    seg_rows, seg_cols = ids_t[0:blk, 0:blk], ids_t[...].T[0:blk, 0:blk]
    ids_t[:, 0:blk] = jnp.broadcast_to(pos_ref[...], (128, blk))
    pos_rows, pos_cols = ids_t[0:blk, 0:blk], ids_t[...].T[0:blk]
    allowed = (seg_rows == seg_cols) & (pos_rows <= pos_cols[:, 0:blk])
    pack_ref[...] = jnp.zeros_like(pack_ref)
    pack_ref[:, 0:blk] = jnp.where(allowed, 1.0, 0.0).astype(BF16)
    pack_ref[:, 128:256] = pos_cols.astype(F32).astype(BF16)

    pack_slot = c * 2 + x % 2
    pack_core = x // 2
    pack_own = c == pack_core

    @pl.when(pack_own)
    def _():
        local(pack_ref, packs.at[pack_slot], ps_r)

    @pl.when(jnp.logical_not(pack_own))
    def _():
        send(pack_ref, packs.at[pack_slot], ps_s.at[0], ps_r, dev(ta=pack_core))

    for d in range(1, NX):
        send(pack_ref, packs.at[pack_slot], ps_s.at[d], ps_r, dev(tb=(x + d) % NX, ta=pack_core))

    for idx in (1, 2):
        issue_w(0, idx, 0)
        issue_w(0, idx, 1)
    swap_wait(x_in.at[0:blk], xs_s, xs_r)
    res[...] = x_in[...].astype(F32)

    def tables():
        wait(packs, ps_r)
        lane = lax.broadcasted_iota(jnp.int32, (8, gq // 2), 1).astype(F32)
        freq = jnp.exp(lane * (-2.0 * math.log(ROPE_BASE) / gq))[0:1]
        for b in range(4):
            ang = packs[b, :, 128:256].astype(F32) * freq
            cos_t[b * blk:(b + 1) * blk, :] = jnp.cos(ang)
            sin_t[b * blk:(b + 1) * blk, :] = jnp.sin(ang)

    def rope(v, rows):
        lo, hi = v[:, 0:128].astype(F32), v[:, 128:256].astype(F32)
        cs, sn = cos_t[rows, :], sin_t[rows, :]
        return jnp.concatenate([lo * cs - hi * sn, hi * cs + lo * sn], axis=1).astype(BF16)

    own_rows = pl.ds(al(c * half, half), half)
    far_rows = pl.ds(al((1 - c) * half, half), half)
    yh, yl = y // 2, y % 2
    sub = half // 2

    def sized(rows):
        return w_at.at[0, 0:rows]

    def hidden():
        return h_buf[...].reshape(tok, 4 * kw)

    def group_at(s):
        return ((x + NX - s) * (1 - c) + (x + s - 1) * c) % NX

    def group_back(s):
        return ((x + s) * (1 - c) + (x + 2 * NX - s - 1) * c) % NX

    back = dev(tb=prv)

    def issue_all(layer, units):
        for idx, part in units:
            issue_w(layer, idx, part)

    def layer_body(layer, carry):
        for g in range(NX):
            for j in range(nch):
                local(wd.at[layer, g * gff + j * CW:g * gff + (j + 1) * CW], wb.at[j, g * CW:(g + 1) * CW], wb_r)
        local(wo.at[layer], wb.at[nch], wb_r)

        r = res[...]
        ssum = jnp.sum(r * r, axis=1, keepdims=True)
        stat = jnp.broadcast_to(ssum, (tb2, 128)).T[0:8]
        stat_own[...] = stat
        for d in range(1, 2 * NX):
            q = (me_plane + d) % (2 * NX)
            send(stat_own, stat_in.at[layer, d - 1], st_s, st_r, dev(tb=q // 2, ta=q % 2))
        issue_all(layer, ((3, 0), (3, 1)))
        wait(stat_in.at[layer], st_r)
        total = stat
        for d in range(2 * NX - 1):
            total = total + stat_in[layer, d]
        mean = jnp.broadcast_to(total[0:1], (128, tb2)).T[:, 0:1] / (kw * 2 * NX)
        gains = gain_ref[:, pl.ds(al(me_plane * kw, 128), kw)].astype(F32)
        gain = jnp.where(layer == 0, gains[0:1], gains[1:2])
        normed = (r * lax.rsqrt(mean + NORM_EPS) * gain).astype(BF16)
        own_cols = pl.ds(al((2 + c) * kw, kw), kw)
        for t in range(2):
            h_buf[yh, t, yl, :, own_cols] = normed[t * blk:(t + 1) * blk]
        mine = h_buf.at[yh, :, yl, :, own_cols]
        far = h_buf.at[yh, :, yl, :, pl.ds(al(c * kw, kw), kw)]
        send(mine, far, h_s, h_r, dev(tb=right, ta=0))
        send(mine, far, h_s, h_r, dev(tb=left, ta=1))
        for d in range(1, NY):
            send(mine, mine, y0_s, y0_r, dev(mp=(y + d) % NY))
        issue_all(layer, ((4, 0), (4, 1), (5, 0), (5, 1), (6, 0), (6, 1)))
        acc[...] = jnp.zeros_like(acc)
        near = h_buf.at[yh, :, yl, :, 0:2 * kw]
        wait(near, h_r)
        for d in range(1, NY):
            send(near, near, y_s, y_r, dev(mp=(y + d) % NY))
        kv_spread(layer)
        wait(sized(3 * tb2), y0_r)
        own_all = h_buf.at[:, :, :, :, own_cols]
        send(own_all, own_all, sb_s, sb_r, sib)
        wait(sized(6 * tb2), y_r)
        wait(sized(tok), sb_r)

        def piece(j, g, p):
            return m_buf.at[j, c, g, p * sub:(p + 1) * sub]

        def share(j, g, p):
            send(piece(j, g, p), piece(j, g, p), d_s, d_r.at[j, p], sib)

        def stage_m_out(j, m):
            m_buf[j, c, group] = m
            for p in range(2):
                blkref = piece(j, group, p)
                send(blkref, blkref, ring_s, ring_r.at[j, 0, p], ring)
                share(j, group, p)

        def stage_r(j, s, p):
            g = group_at(s)
            blkref = piece(j, g, p)
            wait(blkref, ring_r.at[j, s - 1, p])
            if s < NX - 1:
                send(blkref, blkref, ring_s, ring_r.at[j, s, p], ring)
            share(j, g, p)

        def stage_d(j, p):
            wait(m_buf.at[j, 1 - c, :, p * sub:(p + 1) * sub], d_r.at[j, p])
            lhs = jnp.concatenate([
                jnp.concatenate([m_buf[j, hf, g, p * sub:(p + 1) * sub] for g in range(NX)], axis=1) for hf in range(2)
            ], axis=0)
            out = jnp.dot(lhs, wb[j], preferred_element_type=F32)
            for hf in range(2):
                acc[hf * half + p * sub:hf * half + (p + 1) * sub, :] += out[hf * sub:(hf + 1) * sub]

        def stage_p(j):
            wait(w_ml.at[layer, j], w_r.at[layer, j])
            for n in range(2):
                zs[j, :, n * CW:(n + 1) * CW] = jnp.dot(hidden(), w_ml[layer, j, :, n * CW:(n + 1) * CW], preferred_element_type=F32)
            send(zs.at[j, far_rows], zr.at[j], p_s.at[j], p_r.at[j], partner)

        def stage_m(j):
            wait(zr.at[j], p_r.at[j])
            z = zs[j, own_rows, :] + zr[j]
            gate = z[:, 0:CW].astype(BF16).astype(F32)
            up = z[:, CW:2 * CW].astype(BF16).astype(F32)
            stage_m_out(j, (jax.nn.silu(gate) * up).astype(BF16))

        def attn_p():
            wait(w_at.at[layer, 0:(4 * kw * gq + 2 * kw * gkv) // (gq + gkv)], wa_r.at[layer])
            wait(w_at.at[layer, 0:6 * qr, gq:gq + gkv], kvy_r)
            za[...] = jnp.dot(hidden(), w_at[layer], preferred_element_type=F32)
            send(za.at[far_rows, 0:gq], zar, p_s.at[nch], p_r.at[nch], partner)
            send(za.at[pl.ds(al((1 - c) * half + y * blk, blk), blk), gq:gq + gkv], zkv, kvp_s, kvp_r, partner)

        yb = pl.ds(al(y * blk, blk), blk)

        def attn_m():
            wait(zkv, kvp_r)
            kv_buf[group, yb, :] = (za[pl.ds(al(c * half + y * blk, blk), blk), gq:gq + gkv] + zkv[...]).astype(BF16)
            send(kv_buf.at[group, yb], kv_buf.at[group, yb], kv_s, kv_r.at[0], back)
            wait(zar, p_r.at[nch])
            q_buf[...] = (za[own_rows, 0:gq] + zar[...]).astype(BF16)

        def attn_r(s):
            g = group_back(s)
            blkref = kv_buf.at[g, yb]
            wait(blkref, kv_r.at[s - 1])
            if s < NX - 1:
                send(blkref, blkref, kv_s, kv_r.at[s], back)
            else:
                for d in range(1, NY):
                    send(kv_buf.at[:, yb], kv_buf.at[:, yb], kvz_s, kvz_r, dev(mp=(y + d) % NY))

        def attn_core():
            wait(kv_buf.at[0:NX - 1], kvz_r)
            outs = []
            for b in range(4):
                rows = slice(b * blk, (b + 1) * blk)
                q = rope(q_buf[rows, :], rows)
                k = rope(jnp.concatenate([kv_buf[0, rows, :], kv_buf[1, rows, :]], axis=1), rows)
                v = jnp.concatenate([kv_buf[2, rows, :], kv_buf[3, rows, :]], axis=1)
                scores = lax.dot_general(q, k, (((1,), (1,)), ((), ())), preferred_element_type=F32) * (gq ** -0.5)
                scores = jnp.where(packs[b, :, 0:blk].astype(F32) > 0.5, scores, -1e30)
                ex = jnp.exp(scores - jnp.max(scores, axis=1, keepdims=True))
                prob = (ex / jnp.sum(ex, axis=1, keepdims=True)).astype(BF16)
                outs.append(jnp.dot(prob, v, preferred_element_type=F32).astype(BF16))
            stage_m_out(nch, jnp.concatenate(outs, axis=0))

        last = nch - 1
        attn_p()
        for j in range(nch):
            stage_p(j)
        pl.when(layer == 0)(tables)
        attn_m()
        stage_m(0)
        attn_r(1)
        stage_m(1)
        attn_r(2)
        stage_m(2)
        attn_r(3)
        stage_m(3)
        attn_core()
        for j in range(4, nch):
            stage_m(j)
        wait(sized(tok), sb_s)
        wait(wb, wb_r)
        order = (0, 1, 2, 3, nch) + tuple(range(4, nch))
        up, dn, op = (y + 1) % NY, (y + NY - 1) % NY, (y + 2) % NY
        cuts = ((0, 0, blk), (1, 0, blk // 2), (1, blk // 2, blk // 2))

        def part(block, k, second, rows):
            p, off, size = cuts[k]
            return pl.ds(al((block // 2) * half + p * sub + (block % 2) * blk + off + second * (size // 2), size // 2), rows)

        def span(k, second=None):
            p, off, size = cuts[k]
            first = p * blk + off
            if second is None:
                return slice(first, first + size)
            return slice(first + second * size // 2, first + (second + 1) * size // 2)

        def relay_span(k):
            p, off, size = cuts[k]
            return slice((p * blk + off) // 2, (p * blk + off + size) // 2)

        def to_y(rows, dst, k, to):
            send(acc.at[rows], dst, rs_s.at[k], rs_r.at[k], dev(mp=to))

        def sum_relay(k):
            hb = cuts[k][2] // 2
            send(acc.at[part(op, k, 0, hb)], rl_in.at[0, relay_span(k)], rl_s.at[k, 0], rl_r.at[k, 0], dev(mp=up))
            send(acc.at[part(op, k, 1, hb)], rl_in.at[1, relay_span(k)], rl_s.at[k, 1], rl_r.at[k, 1], dev(mp=dn))

        def sum_direct(k):
            hb = cuts[k][2] // 2
            for i in range(2):
                wait(rl_in.at[i, relay_span(k)], rl_s.at[k, i])
            to_y(part(up, k, 1, hb), rs_in.at[0, span(k, 1)], k, up)
            to_y(part(dn, k, 0, hb), rs_in.at[1, span(k, 0)], k, dn)

        def sum_pass(k):
            hb = cuts[k][2] // 2
            wait(rl_in.at[0, relay_span(k)], rl_r.at[k, 0])
            acc[part(up, k, 0, hb), :] += rl_in[0, relay_span(k)]
            to_y(part(up, k, 0, hb), rs_in.at[0, span(k, 0)], k, up)
            wait(rl_in.at[1, relay_span(k)], rl_r.at[k, 1])
            acc[part(dn, k, 1, hb), :] += rl_in[1, relay_span(k)]
            to_y(part(dn, k, 1, hb), rs_in.at[1, span(k, 1)], k, dn)

        def sum_end(k):
            p, off, size = cuts[k]
            wait(rs_in.at[0:2, span(k)], rs_r.at[k])
            res[span(k), :] = res[span(k), :] + (acc[part(y, k, 0, size), :] + rs_in[0, span(k)] + rs_in[1, span(k)])

            @pl.when(layer == layers - 1)
            def _():
                swap_send(p, res.at[span(k)], out_ref.at[off:off + size, pl.ds(al(c * kw, kw), kw)], f_s, f_r)

        for s, p in ((1, 0), (2, 0), (1, 1)):
            for j in order:
                stage_r(j, s, p)
        for i, j in enumerate(order):
            stage_r(j, 3, 0)
            if i > 0:
                stage_d(order[i - 1], 0)
        stage_d(order[-1], 0)
        sum_relay(0)
        for j in order:
            stage_r(j, 2, 1)

        @pl.when(layer < layers - 1)
        def _():
            issue_all(layer + 1, ((0, 0), (0, 1), (1, 0), (1, 1), (2, 0), (2, 1)))

        sum_direct(0)
        stage_r(order[0], 3, 1)
        for i, j in enumerate(order[1:]):
            stage_r(j, 3, 1)
            stage_d(order[i], 1)
            if i == 0:
                sum_pass(0)
            if i == 5:
                sum_end(0)
        stage_d(order[-1], 1)
        sum_relay(1)
        sum_relay(2)
        sum_direct(1)
        sum_pass(1)
        sum_direct(2)
        sum_pass(2)
        sum_end(1)
        sum_end(2)

        wait(stat_in.at[layer], st_s)
        wait(sized(2 * tb2), h_s)
        wait(sized(3 * tb2), y0_s)
        wait(sized(6 * tb2), y_s)
        for j in range(nch):
            wait(zr.at[j], p_s.at[j])
        wait(zar, p_s.at[nch])
        wait(kv_buf.at[0, 0:3 * blk], kv_s)
        wait(kv_buf.at[0:NX - 1], kvz_s)
        wait(zkv, kvp_s)
        wait(w_at.at[layer, 0:2 * qr, gq:gq + gkv], kvx_s.at[layer])
        wait(w_at.at[layer, 0:6 * qr, gq:gq + gkv], kvy_s)
        wait(m_buf.at[:, 0, 0:NX - 1], ring_s)
        wait(m_buf.at[:, 0], d_s)
        for k in range(3):
            wait(acc.at[0:2 * cuts[k][2]], rs_s.at[k])
        wait(w_at.at[layer, 0:(3 * kw * gq + kw * gkv) // (gq + gkv)], wa_s.at[layer])
        wait(w_ml.at[layer, :, 0:3 * kw], w_s.at[layer])
        return carry

    lax.fori_loop(0, layers, layer_body, 0)

    swap_wait(res.at[0:blk], f_s, f_r)

    @pl.when(jnp.logical_not(pack_own))
    def _():
        wait(pack_ref, ps_s.at[0])

    for d in range(1, NX):
        wait(pack_ref, ps_s.at[d])


def solution(mesh):
    def device_body(x_loc, seg_ids, pos_ids, w_q, w_k, w_v, w_gate, w_up, w_out, w_down, gain):
        blk, width_loc = x_loc.shape
        layers, kw, _ = w_q.shape
        head_dim = w_k.shape[-1]
        gq = w_q.shape[-1] // NX
        gff = w_gate.shape[-1] // NX
        gkv = 2 * head_dim // NX
        nch = gff // CW
        tok, half, tb2 = 8 * blk, 4 * blk, 2 * blk
        kg = 4 * kw
        half_dim = head_dim // 2
        hbm = pl.BlockSpec(memory_space=pl.ANY)
        dma = pltpu.SemaphoreType.DMA
        return pl.pallas_call(
            functools.partial(kernel, (layers, blk, kw, gq, gkv, gff)),
            out_shape=jax.ShapeDtypeStruct((blk, width_loc), F32),
            in_specs=[hbm] * 11,
            out_specs=hbm,
            scratch_shapes=[
                pltpu.VMEM((layers, kg, gq + gkv), BF16),
                pltpu.VMEM((layers, nch, kg, 2 * CW), BF16),
                pltpu.VMEM((nch + 1, NX * CW, kw), BF16),
                pltpu.VMEM((nch, tok, 2 * CW), F32),
                pltpu.VMEM((nch, half, 2 * CW), F32),
                pltpu.VMEM((tok, gq + gkv), F32),
                pltpu.VMEM((half, gq), F32),
                pltpu.VMEM((blk, gkv), F32),
                pltpu.VMEM((nch + 1, 2, NX, half, CW), BF16),
                pltpu.VMEM((2, 2, 2, blk, kg), BF16),
                pltpu.VMEM((tok, kw), F32),
                pltpu.VMEM((tb2, kw), F32),
                pltpu.VMEM((NX, half, gkv), BF16),
                pltpu.VMEM((half, gq), BF16),
                pltpu.VMEM((half, half_dim), F32),
                pltpu.VMEM((half, half_dim), F32),
                pltpu.VMEM((4, blk, 256), BF16),
                pltpu.VMEM((8, tb2), F32),
                pltpu.VMEM((layers, 2 * NX - 1, 8, tb2), F32),
                pltpu.VMEM((2, tb2, kw), F32),
                pltpu.VMEM((2, blk, kw), F32),
                pltpu.VMEM((tb2, kw), BF16),
                pltpu.VMEM((blk, 256), BF16),
                pltpu.VMEM((128, 128), jnp.int32),
                pltpu.VMEM((1, blk), jnp.int32),
                pltpu.VMEM((1, blk), jnp.int32),
                pltpu.VMEM(gain.shape, BF16),
                dma((2,)), dma((2,)), dma((NX,)), dma(()),
                dma((layers,)), dma((layers,)), dma((layers, nch)), dma((layers,)), dma(()),
                dma((nch + 1,)), dma((nch + 1,)),
                dma(()), dma((nch + 1, NX - 1, 2)), dma(()), dma((nch + 1, 2)),
                dma(()), dma((NX - 1,)),
            ] + [dma(())] * 10 + [
                dma((3,)), dma((3,)), dma((3, 2)), dma((3, 2)), dma((2,)), dma((2,)), dma((layers,)), dma((layers,)),
            ] + [dma(())] * 6 + [dma((3,))],
            compiler_params=pltpu.CompilerParams(collective_id=0, has_side_effects=True, vmem_limit_bytes=60 * 1024 * 1024),
        )(x_loc, seg_ids[None], pos_ids[None], gain, w_q, w_k, w_v, w_gate, w_up, w_out, w_down)

    col_spec = P(None, PLANE_AXES, "mp")
    kv_spec = P(None, PLANE_AXES, None)
    row_spec = P(None, "mp", PLANE_AXES)
    return jax.shard_map(
        device_body,
        mesh=mesh,
        in_specs=(P(TOKEN_AXES, "mp"), P(TOKEN_AXES), P(TOKEN_AXES), col_spec, kv_spec, kv_spec, col_spec, col_spec, row_spec, row_spec, P(None, None)),
        out_specs=P(TOKEN_AXES, "mp"),
        check_vma=False,
    )
```
